32 devices in a mesh: gz: 16 (over z, x, core), gy: 2 (over y).
Axes of the slice: x: 2, y: 2, z: 4, core: 2. Of those that a mesh axis runs over, the one named last changes fastest.
Arguments:
- spread_weights: float32 [64, 32768], P(None, ('gz', 'gy')), may hold values from -6 to 6
- spread_base: int32 [3, 32768], P(None, ('gz', 'gy')), may hold values from 0 to 383, as said below
- qm_base: int32 [3, 4096], P(None, ('gz', 'gy')), may hold values from 0 to 383, as said below
- qm_frac: float32 [3, 4096], P(None, ('gz', 'gy')), may hold values from 0 to 1
- qm_charge: float32 [4096], P(('gz', 'gy')), may hold values from -3 to 3
Outputs:
- qm_forces: float32 [3, 4096], P(None, ('gz', 'gy'))
The draws below stay inside these ranges and needn't reach their ends.
Inputs may be any that keep to these rules, and one draw needn't show every extreme that they name: For point charge j let d = j // 1024, p = d // 2 and q = d % 2; then spread_base[0, j] lies in [p * 24, (p + 1) * 24) and spread_base[1, j] in [q * 192, (q + 1) * 192); spread_base[2, j] is any cell. For quantum-region atom i let d = i // 128, p = d // 2 and q = d % 2; then qm_base[0, i] lies in [p * 24, (p + 1) * 24) and qm_base[1, i] in [q * 192, (q + 1) * 192); qm_base[2, i] is any cell.
All inputs are finite; a program needn't handle non-finite values.
Results may differ from the reference program's by a relative error of at most 0.0003.
Values sent between devices are 32-bit elements; how exact they have to be, the bound alone decides.
No kernel may reach another device: no remote copies, remote signals or barrier semaphores. Data moves between devices by JAX's collectives and lax.ppermute only.
A program may use at most 256 MiB of HBM per device.

```python
import math
import jax
import jax.numpy as jnp

GRID = 384
ORDER = 4
ATOMS_DEV = 1024
QM_DEV = 128
ZLOC = 24
YLOC = 192
ATOMS = 32768
QMS = 4096


def place_bases(key, total, per_device):
    index = jnp.arange(total, dtype=jnp.int32)
    device = index // per_device
    groups = GRID // YLOC
    z_part = device // groups
    y_part = device % groups
    key_z, key_y, key_x = jax.random.split(key, 3)
    first_z = z_part * ZLOC + jax.random.randint(key_z, (total,), 0, ZLOC, dtype=jnp.int32)
    first_y = y_part * YLOC + jax.random.randint(key_y, (total,), 0, YLOC, dtype=jnp.int32)
    first_x = jax.random.randint(key_x, (total,), 0, GRID, dtype=jnp.int32)
    return jnp.stack([first_z, first_y, first_x]).astype(jnp.int32)


def draw_spread_base(key, part):
    return place_bases(jax.random.fold_in(key, 11), ATOMS, ATOMS_DEV)


def draw_qm_base(key, part):
    return place_bases(jax.random.fold_in(key, 23), QMS, QM_DEV)


def block_scale(own_key, extent, cuts, low, top_value):
    loudness, own = 1.0, jax.random.fold_in(own_key, 6)
    for position, blocks in cuts:
        draws = jnp.exp(jax.random.uniform(jax.random.fold_in(own, position), (blocks,), jnp.float32, low / len(cuts), top_value / len(cuts)))
        loudness = loudness * jnp.repeat(draws, extent[position] // blocks).reshape([-1 if axis == position else 1 for axis in range(len(extent))])
    return loudness


def normal_values(rng, shape, deviation, limit, shards=(), kind=jnp.bfloat16):
    drawn = jax.random.normal(rng, shape, jnp.float32) * deviation
    if len(shards) > 0:
        drawn = block_scale(rng, shape, shards, -0.22, 0.18) * drawn
    return jnp.clip(drawn, min=-limit, max=limit).astype(kind)


def setup_inputs(seed: int = 0) -> dict:
    keys = jax.random.split(jax.random.key(seed), 6)
    return {
        "spread_weights": normal_values(keys[0], (ORDER * ORDER * ORDER, ATOMS), 1.0, 6.0, ((1, 32),), jnp.float32),
        "spread_base": draw_spread_base(jax.random.fold_in(keys[5], 71), 0),
        "qm_base": draw_qm_base(jax.random.fold_in(keys[5], 71), 0),
        "qm_frac": jnp.clip(1.0 * jax.random.uniform(keys[3], (3, QMS), jnp.float32) ** block_scale(keys[3], (3, QMS), ((1, 32),), -0.2, 0.2), 0.0, 1.0),
        "qm_charge": normal_values(keys[4], (QMS,), 0.5, 3.0, ((0, 32),), jnp.float32),
    }


SPLITTING = 0.8


def moduli(index, points):
    signed = jnp.where(index < points // 2, index, index - points).astype(jnp.float32) / points
    spline = 2.0 / 3.0 + jnp.cos((2.0 * math.pi / points) * index.astype(jnp.float32)) / 3.0
    return signed * signed, 1.0 / (spline * spline), index == points // 2


def influence(first, second, third, points):
    sq_one, mod_one, edge_one = moduli(first, points)
    sq_two, mod_two, edge_two = moduli(second, points)
    sq_three, mod_three, edge_three = moduli(third, points)
    total = sq_one + sq_two + sq_three
    safe = jnp.where(total > 0.0, total, 1.0)
    value = mod_one * mod_two * mod_three * jnp.exp(-(math.pi * math.pi / (SPLITTING * SPLITTING)) * total) / (math.pi * safe)
    keep = (total > 0.0) & jnp.logical_not(edge_one | edge_two | edge_three)
    return jnp.where(keep, value, 0.0)


def spline_weights(frac):
    remain = 1.0 - frac
    square = frac * frac
    cubed = square * frac
    values = jnp.stack([remain * remain * remain / 6.0, (3.0 * cubed - 6.0 * square + 4.0) / 6.0,
                        (-3.0 * cubed + 3.0 * square + 3.0 * frac + 1.0) / 6.0, cubed / 6.0])
    slopes = jnp.stack([-0.5 * remain * remain, (3.0 * square - 4.0 * frac) / 2.0,
                        (-3.0 * square + 2.0 * frac + 1.0) / 2.0, 0.5 * square])
    return values, slopes


def forces_from(patch, qm_frac, qm_charge):
    w_z, d_z = spline_weights(qm_frac[0])
    w_y, d_y = spline_weights(qm_frac[1])
    w_x, d_x = spline_weights(qm_frac[2])

    def contract(first, second, third):
        return jnp.sum(patch * (first[:, None, None, :] * second[None, :, None, :] * third[None, None, :, :]), axis=(0, 1, 2))

    return jnp.stack([-qm_charge * contract(d_z, w_y, w_x), -qm_charge * contract(w_z, d_y, w_x),
                      -qm_charge * contract(w_z, w_y, d_x)])


def reference(spread_weights, spread_base, qm_base, qm_frac, qm_charge):
    points = GRID
    offsets = jnp.arange(ORDER * ORDER * ORDER, dtype=jnp.int32)
    off_z = offsets // (ORDER * ORDER)
    off_y = (offsets // ORDER) % ORDER
    off_x = offsets % ORDER
    flat_index = (((spread_base[0][None, :] + off_z[:, None]) % points) * points
                  + (spread_base[1][None, :] + off_y[:, None]) % points) * points + (spread_base[2][None, :] + off_x[:, None]) % points
    charge = jnp.zeros((points * points * points,), jnp.float32).at[flat_index.reshape(-1)].add(spread_weights.reshape(-1))
    charge = charge.reshape(points, points, points)
    spectrum = jnp.fft.fftn(charge)
    index = jnp.arange(points, dtype=jnp.int32)
    green = influence(index[:, None, None], index[None, :, None], index[None, None, :], points)
    potential = jnp.real(jnp.fft.ifftn(spectrum * green)).astype(jnp.float32)
    shifts_up = jnp.arange(ORDER, dtype=jnp.int32)[:, None]
    cell_z = (qm_base[0][None, :] + shifts_up) % points
    cell_y = (qm_base[1][None, :] + shifts_up) % points
    cell_x = (qm_base[2][None, :] + shifts_up) % points
    patch = potential[cell_z[:, None, None, :], cell_y[None, :, None, :], cell_x[None, None, :, :]]
    return forces_from(patch, qm_frac, qm_charge)
```

```python
import math

import jax
import jax.numpy as jnp
import numpy as np
from jax import lax
from jax.experimental import pallas as pl
from jax.experimental.pallas import tpu as pltpu
from jax.sharding import PartitionSpec as P

GRID = 384
ORDER = 4
SPLITTING = 0.8
AXES = ("gz", "gy")
RADIX = 3


def round_up(value, unit):
    return -(-value // unit) * unit


def window_start(z_part, z_local):
    return pl.multiple_of(z_part * z_local // 8 * 8, 8)


def spline_weights(frac):
    remain = 1.0 - frac
    square = frac * frac
    cubed = square * frac
    values = [
        remain * remain * remain / 6.0,
        (3.0 * cubed - 6.0 * square + 4.0) / 6.0,
        (-3.0 * cubed + 3.0 * square + 3.0 * frac + 1.0) / 6.0,
        cubed / 6.0,
    ]
    slopes = [
        -0.5 * remain * remain,
        (3.0 * square - 4.0 * frac) / 2.0,
        (-3.0 * square + 2.0 * frac + 1.0) / 2.0,
        0.5 * square,
    ]
    return values, slopes


def sine_of_turns(turn):
    square = turn * turn
    total = jnp.full_like(turn, 0.0)
    for power in range(6, -1, -1):
        term = (-1.0) ** power * (2.0 * math.pi) ** (2 * power + 1) / math.factorial(2 * power + 1)
        total = total * square + term
    return total * turn


def cos_sin_of_turns(turn):
    folded = jnp.minimum(jnp.maximum(turn, -0.5 - turn), 0.5 - turn)
    return sine_of_turns(0.25 - jnp.abs(turn)), sine_of_turns(folded)


def halves(value):
    high = value.astype(jnp.bfloat16)
    low = (value - high.astype(jnp.float32)).astype(jnp.bfloat16)
    return high, low


def dot(left, right, contract=((1,), (0,))):
    return lax.dot_general(left, right, (contract, ((), ())), preferred_element_type=jnp.float32)


def x_phases(cells, kx_column, points):
    product = kx_column * cells
    turn = product * (1.0 / points)
    rest = product - points * jnp.floor(turn + 0.5)
    return cos_sin_of_turns(rest * (1.0 / points))


def spread_kernel(kx_ref, rec_ref, out_ref, *, points, z_local, y_local, count_y, kx_here, z_rows, y_rows):
    step = pl.program_id(0)
    z_part = step // count_y
    y_part = step % count_y
    atoms = rec_ref.shape[2]
    cells = ORDER**3

    @pl.when(step == 0)
    def _():
        out_ref[...] = jnp.zeros_like(out_ref)

    start = window_start(z_part, z_local)
    first_z = start.astype(jnp.float32)
    first_y = (y_part * y_local).astype(jnp.float32)
    local_z = (rec_ref[0, cells : cells + 1, :] - first_z).astype(jnp.int32)
    local_y = (rec_ref[0, cells + 1 : cells + 2, :] - first_y).astype(jnp.int32)
    x_cell = rec_ref[0, cells + 2 : cells + 3, :]
    kx_column = kx_ref[:, 0:1]
    base_cos, base_sin = x_phases(x_cell, kx_column, points)
    phase_re, phase_im = [base_cos], [-base_sin]
    for c in range(1, ORDER):
        turn_cos = kx_ref[:, 2 * c : 2 * c + 1]
        turn_sin = kx_ref[:, 2 * c + 1 : 2 * c + 2]
        phase_re.append(base_cos * turn_cos - base_sin * turn_sin)
        phase_im.append(-(base_sin * turn_cos + base_cos * turn_sin))
    z_iota = lax.broadcasted_iota(jnp.int32, (z_rows, atoms), 0)
    offset_z = z_iota - local_z
    y_iota = lax.broadcasted_iota(jnp.int32, (y_rows, atoms), 0)
    offset_y = y_iota - local_y
    masks = [offset_z == a for a in range(ORDER)]
    total = None
    for b in range(ORDER):
        pieces = [[], []]
        lines = []
        for a in range(ORDER):
            re = im = None
            for c in range(ORDER):
                row = a * ORDER * ORDER + b * ORDER + c
                weight = rec_ref[0, row : row + 1, :]
                re = weight * phase_re[c] if re is None else re + weight * phase_re[c]
                im = weight * phase_im[c] if im is None else im + weight * phase_im[c]
            lines.append((re, im))
        rows_hi, rows_lo = [], []
        for part in range(2):
            for k in range(kx_here):
                value = jnp.zeros((z_rows, atoms), jnp.float32)
                for a in range(ORDER):
                    value = jnp.where(masks[a], lines[a][part][k : k + 1, :], value)
                high, low = halves(value)
                rows_hi.append(high)
                rows_lo.append(low)
        hits = (offset_y == b).astype(jnp.float32).astype(jnp.bfloat16)
        stacked = jnp.concatenate(rows_hi + rows_lo, axis=0)
        product = dot(stacked, hits, ((1,), (1,)))
        total = product if total is None else total + product
    half = 2 * kx_here * z_rows
    for n in range(2 * kx_here):
        piece = total[n * z_rows : (n + 1) * z_rows] + total[half + n * z_rows : half + (n + 1) * z_rows]
        out_ref[y_part, n, pl.ds(start, z_rows), :] += piece


def split_dot(value, high, low):
    top, rest = halves(value)
    return dot(top, high) + (dot(rest, high) + dot(top, low))


def split_dot_left(high, low, value):
    top, rest = halves(value)
    return dot(high, top) + (dot(high, rest) + dot(low, top))


HALF_ROOT = math.sqrt(3.0) / 2.0


def three_way(parts, sign):
    (ar, ai), (br, bi), (cr, ci) = parts
    sum_r, sum_i = br + cr, bi + ci
    dif_r, dif_i = (br - cr) * HALF_ROOT, (bi - ci) * HALF_ROOT
    mid_r, mid_i = ar - 0.5 * sum_r, ai - 0.5 * sum_i
    return [
        (ar + sum_r, ai + sum_i),
        (mid_r - sign * dif_i, mid_i + sign * dif_r),
        (mid_r + sign * dif_i, mid_i - sign * dif_r),
    ]


def turned(value, cosine, sine, sign):
    re, im = value
    return (re * cosine - sign * (im * sine), im * cosine + sign * (re * sine))


def transform_kernel(
    scal_ref, re_ref, im_ref, right_hi, right_lo, left_hi, left_lo, tw_row, tw_col, row_ref, col_ref,
    out_ref, *, points, y_local, count_y, third,
):
    index = pl.program_id(0)
    z_pad = re_ref.shape[2]
    y_rows = re_ref.shape[3]

    def whole(ref):
        plane = None
        for q in range(count_y):
            piece = ref[q, 0]
            body = piece[:points]
            spare = z_pad - points
            body = jnp.concatenate([body[:spare] + piece[points:], body[spare:]], axis=0)
            if y_rows < points:
                body = jnp.concatenate(
                    [body, jnp.zeros((points, points - y_rows), jnp.float32)], axis=1
                )
            if q > 0:
                body = pltpu.roll(body, q * y_local, 1)
            plane = body if plane is None else plane + body
        return plane

    def lanes(value, part):
        return tuple(v[:, part * third : (part + 1) * third] for v in value)

    def rows(value, part):
        return tuple(v[part * third : (part + 1) * third] for v in value)

    plane = (whole(re_ref), whole(im_ref))
    parts = three_way([lanes(plane, n) for n in range(RADIX)], -1.0)
    done = []
    for n, part in enumerate(parts):
        if n > 0:
            part = turned(part, tw_row[2 * n : 2 * n + 1, :], tw_row[2 * n + 1 : 2 * n + 2, :], -1.0)
        done.append(split_dot(jnp.concatenate(part, axis=1), right_hi[...], right_lo[...]))
    parts = three_way(
        [
            (
                jnp.concatenate([d[n * third : (n + 1) * third, :third] for d in done], axis=1),
                jnp.concatenate([d[n * third : (n + 1) * third, third:] for d in done], axis=1),
            )
            for n in range(RADIX)
        ],
        -1.0,
    )
    scale = scal_ref[index, 0]
    square = scal_ref[index, 1]
    back = []
    for n, part in enumerate(parts):
        if n > 0:
            cosine = jnp.concatenate([tw_col[2 * n]] * RADIX, axis=1)
            sine = jnp.concatenate([tw_col[2 * n + 1]] * RADIX, axis=1)
            part = turned(part, cosine, sine, -1.0)
        spectrum = split_dot_left(left_hi[...], left_lo[...], jnp.concatenate(part, axis=0))
        col_factor = jnp.concatenate([col_ref[0, n * third : (n + 1) * third, :]] * RADIX, axis=1)
        col_square = jnp.concatenate([col_ref[1, n * third : (n + 1) * third, :]] * RADIX, axis=1)
        total = col_square + row_ref[1:2, :] + square
        safe = jnp.where(total > 0.0, total, 1.0)
        green = jnp.where(total > 0.0, col_factor * row_ref[0:1, :] * scale / (math.pi * safe), 0.0)
        swapped = jnp.concatenate([spectrum[third:] * green, spectrum[:third] * green], axis=0)
        result = split_dot_left(left_hi[...], left_lo[...], swapped)
        part = (result[third:], result[:third])
        if n > 0:
            part = turned(part, cosine, sine, 1.0)
        back.append(part)
    back = three_way(back, 1.0)
    plane = tuple(jnp.concatenate([b[i] for b in back], axis=0) for i in range(2))
    parts = []
    for n in range(RADIX):
        re, im = lanes(plane, n)
        result = split_dot(jnp.concatenate([im, re], axis=1), right_hi[...], right_lo[...])
        part = (result[:, third:], result[:, :third])
        if n > 0:
            part = turned(part, tw_row[2 * n : 2 * n + 1, :], tw_row[2 * n + 1 : 2 * n + 2, :], 1.0)
        parts.append(part)
    parts = three_way(parts, 1.0)
    spare = out_ref.shape[2] - points
    for i in range(2):
        value = jnp.concatenate([p[i] for p in parts], axis=1)
        out_ref[i, 0, :points, :] = value
        out_ref[i, 0, points:, :] = value[:spare]


def force_kernel(kx_ref, qm_ref, pot_ref, out_ref, *, points, z_local, count_y, kx_here, z_rows):
    step = pl.program_id(0)
    z_part = step // count_y
    atoms = qm_ref.shape[2]
    start = window_start(z_part, z_local)
    first_z = start.astype(jnp.float32)
    local_z = (qm_ref[0, 0:1, :] - first_z).astype(jnp.int32)
    cell_y = qm_ref[0, 1:2, :].astype(jnp.int32)
    x_cell = qm_ref[0, 2:3, :]
    w_z, d_z = spline_weights(qm_ref[0, 3:4, :])
    w_y, d_y = spline_weights(qm_ref[0, 4:5, :])
    w_x, d_x = spline_weights(qm_ref[0, 5:6, :])

    def placed(offset, weights):
        value = jnp.zeros(offset.shape, jnp.float32)
        for a in range(ORDER):
            value = jnp.where(offset == a, weights[a], value)
        return value

    offset_z = lax.broadcasted_iota(jnp.int32, (z_rows, atoms), 0) - local_z
    plane_w, plane_d = placed(offset_z, w_z), placed(offset_z, d_z)
    offset_y = lax.broadcasted_iota(jnp.int32, (points, atoms), 0) - cell_y
    offset_y = jnp.where(offset_y < 0, offset_y + points, offset_y)
    row_hi, row_lo = halves(jnp.concatenate([placed(offset_y, w_y), placed(offset_y, d_y)], axis=1))
    base_cos, base_sin = x_phases(x_cell, kx_ref[:, 0:1], points)
    line_w = [w_x[0] * base_cos, w_x[0] * base_sin]
    line_d = [d_x[0] * base_cos, d_x[0] * base_sin]
    for c in range(1, ORDER):
        turn_cos = kx_ref[:, 2 * c : 2 * c + 1]
        turn_sin = kx_ref[:, 2 * c + 1 : 2 * c + 2]
        cosine = base_cos * turn_cos - base_sin * turn_sin
        sine = base_sin * turn_cos + base_cos * turn_sin
        line_w = [line_w[0] + w_x[c] * cosine, line_w[1] + w_x[c] * sine]
        line_d = [line_d[0] + d_x[c] * cosine, line_d[1] + d_x[c] * sine]
    force = [jnp.zeros((1, atoms), jnp.float32) for _ in range(3)]
    window = jnp.concatenate(
        [pot_ref[i, k, pl.ds(start, z_rows), :] for k in range(kx_here) for i in range(2)], axis=0
    )
    top, rest = halves(window)
    along = dot(top, row_hi) + (dot(rest, row_hi) + dot(top, row_lo))
    for k in range(kx_here):
        for i in range(2):
            n = (2 * k + i) * z_rows
            plain, sloped = along[n : n + z_rows, :atoms], along[n : n + z_rows, atoms:]
            sign = 1.0 if i == 0 else -1.0
            sum_z = jnp.sum(plain * plane_d, axis=0, keepdims=True)
            sum_y = jnp.sum(sloped * plane_w, axis=0, keepdims=True)
            sum_x = jnp.sum(plain * plane_w, axis=0, keepdims=True)
            across = line_w[i][k : k + 1, :] * sign
            force[0] += sum_z * across
            force[1] += sum_y * across
            force[2] += sum_x * (line_d[i][k : k + 1, :] * sign)
    out_ref[0] = jnp.concatenate(force, axis=0)


def tables(points):
    third = points // RADIX
    index = np.arange(third)
    angle = 2.0 * np.pi / third * (np.outer(index, index) % third)
    cosine, sine = np.cos(angle), np.sin(angle)
    right = np.block([[cosine, -sine], [sine, cosine]])
    left = np.block([[cosine, sine], [-sine, cosine]])

    def split(matrix):
        value = jnp.asarray(matrix, jnp.float32)
        high = jnp.asarray(matrix.astype(jnp.bfloat16))
        low = jnp.asarray((matrix - matrix.astype(jnp.bfloat16).astype(np.float64)).astype(jnp.bfloat16))
        return high, low

    turn = 2.0 * np.pi / points * np.outer(np.arange(RADIX), index)
    twiddle = np.stack([np.cos(turn), np.sin(turn)], axis=1).reshape(2 * RADIX, third).astype(np.float32)
    tw_row = jnp.asarray(twiddle)
    tw_col = jnp.asarray(np.broadcast_to(twiddle[:, :, None], (2 * RADIX, third, third)).copy())
    slots = (RADIX * np.arange(third)[None, :] + np.arange(RADIX)[:, None]).reshape(-1)
    factor, square = factors(slots, points)
    row = jnp.asarray(np.stack([factor, square]).astype(np.float32))
    col = jnp.asarray(
        np.broadcast_to(np.stack([factor, square])[:, :, None], (2, points, third)).astype(np.float32)
    )
    return split(right) + split(left) + (tw_row, tw_col, row, col)


def factors(index, points):
    signed = np.where(index < points // 2, index, index - points) / points
    spline = 2.0 / 3.0 + np.cos(2.0 * np.pi * index / points) / 3.0
    factor = np.exp(-((np.pi / SPLITTING) ** 2) * signed**2) / spline**2
    return np.where(index == points // 2, 0.0, factor), signed**2


def shards(spread_weights, spread_base, qm_base, qm_frac, qm_charge):
    points = GRID
    count_z = lax.axis_size("gz")
    count_y = lax.axis_size("gy")
    devices = count_z * count_y
    z_local = points // count_z
    y_local = points // count_y
    kx_here = -(-(points // 2) // devices)
    here = lax.axis_index("gz") * count_y + lax.axis_index("gy")
    kx = here * kx_here + jnp.arange(kx_here, dtype=jnp.int32)
    z_rows = round_up(z_local + ORDER - 1 + (0 if z_local % 8 == 0 else 7), 8)
    z_pad = (points - z_local) // 8 * 8 + z_rows
    y_rows = min(round_up(y_local + ORDER - 1, 128), points)

    atoms = spread_weights.shape[1]
    qms = qm_charge.shape[0]
    qm_rows = jnp.concatenate([qm_base.astype(jnp.float32), qm_frac], axis=0).reshape(-1)
    lines = -(-qm_rows.shape[0] // atoms)
    qm_rows = jnp.pad(qm_rows, (0, lines * atoms - qm_rows.shape[0])).reshape(lines, atoms)
    record = jnp.concatenate([spread_weights, spread_base.astype(jnp.float32), qm_rows], axis=0)
    held = round_up(record.shape[0], 8)
    record = jnp.pad(record, ((0, held - record.shape[0]), (0, 0)))
    records = lax.all_gather(record, AXES, axis=0, tiled=False)

    fkx = kx.astype(jnp.float32)
    turn = 2.0 * math.pi / points * ((kx[:, None] * jnp.arange(ORDER)[None, :]) % points).astype(jnp.float32)
    kx_table = jnp.stack([jnp.cos(turn), jnp.sin(turn)], axis=2).reshape(kx_here, 2 * ORDER)
    kx_table = kx_table.at[:, 0].set(fkx)

    spread = pl.pallas_call(
        lambda *refs: spread_kernel(
            *refs, points=points, z_local=z_local, y_local=y_local, count_y=count_y,
            kx_here=kx_here, z_rows=z_rows, y_rows=y_rows,
        ),
        grid=(devices,),
        in_specs=[
            pl.BlockSpec(kx_table.shape, lambda d: (0, 0)),
            pl.BlockSpec((1, held, atoms), lambda d: (d, 0, 0)),
        ],
        out_specs=pl.BlockSpec((count_y, 2 * kx_here, z_pad, y_rows), lambda d: (0, 0, 0, 0)),
        out_shape=jax.ShapeDtypeStruct((count_y, 2 * kx_here, z_pad, y_rows), jnp.float32),
        compiler_params=pltpu.CompilerParams(
            dimension_semantics=("arbitrary",), vmem_limit_bytes=60 * 1024 * 1024
        ),
        name="spread",
    )(kx_table, records)

    signed = fkx / points
    spline = 2.0 / 3.0 + jnp.cos(2.0 * math.pi / points * fkx) / 3.0
    kx_factor = jnp.exp(-((math.pi / SPLITTING) ** 2) * signed * signed) / (spline * spline)
    kx_factor = kx_factor * jnp.where(kx == 0, 1.0, 2.0) / float(points) ** 3
    kx_factor = jnp.where(kx < points // 2, kx_factor, 0.0)
    scalars = jnp.stack([kx_factor, signed * signed], axis=1)
    constants = tables(points)
    third = points // RADIX

    def fixed(array):
        return pl.BlockSpec(array.shape, lambda k, n=array.ndim: (0,) * n)

    block = (count_y, 1, z_pad, y_rows)
    potential = pl.pallas_call(
        lambda *refs: transform_kernel(
            *refs, points=points, y_local=y_local, count_y=count_y, third=third
        ),
        grid=(kx_here,),
        in_specs=[
            pl.BlockSpec(memory_space=pltpu.SMEM),
            pl.BlockSpec(block, lambda k: (0, k, 0, 0)),
            pl.BlockSpec(block, lambda k: (0, k + kx_here, 0, 0)),
        ]
        + [fixed(array) for array in constants],
        out_specs=pl.BlockSpec((2, 1, z_pad, points), lambda k: (0, k, 0, 0)),
        out_shape=jax.ShapeDtypeStruct((2, kx_here, z_pad, points), jnp.float32),
        compiler_params=pltpu.CompilerParams(
            dimension_semantics=("arbitrary",), vmem_limit_bytes=60 * 1024 * 1024
        ),
        name="transform",
    )(scalars, spread, spread, *constants)

    first_line = ORDER**3 + 3
    qm_all = records[:, first_line : first_line + lines, :].reshape(devices, lines * atoms)
    qm_all = qm_all[:, : 6 * qms].reshape(devices, 6, qms)
    partial = pl.pallas_call(
        lambda *refs: force_kernel(
            *refs, points=points, z_local=z_local, count_y=count_y, kx_here=kx_here, z_rows=z_rows
        ),
        grid=(devices,),
        in_specs=[
            pl.BlockSpec(kx_table.shape, lambda d: (0, 0)),
            pl.BlockSpec((1, 6, qms), lambda d: (d, 0, 0)),
            pl.BlockSpec((2, kx_here, z_pad, points), lambda d: (0, 0, 0, 0)),
        ],
        out_specs=pl.BlockSpec((1, 3, qms), lambda d: (d, 0, 0)),
        out_shape=jax.ShapeDtypeStruct((devices, 3, qms), jnp.float32),
        compiler_params=pltpu.CompilerParams(
            dimension_semantics=("arbitrary",), vmem_limit_bytes=60 * 1024 * 1024
        ),
        name="forces",
    )(kx_table, qm_all, potential)
    moved = lax.all_to_all(partial, AXES, split_axis=0, concat_axis=0, tiled=True)
    return -qm_charge[None, :] * jnp.sum(moved, axis=0)


def solution(mesh):
    in_specs = (
        P(None, AXES),
        P(None, AXES),
        P(None, AXES),
        P(None, AXES),
        P(AXES),
    )
    out_specs = P(None, AXES)
    return jax.shard_map(shards, mesh=mesh, in_specs=in_specs, out_specs=out_specs, check_vma=False)
```

```python
import math

import jax
import jax.numpy as jnp
import numpy as np
from jax import lax
from jax.experimental import pallas as pl
from jax.experimental.pallas import tpu as pltpu
from jax.sharding import PartitionSpec as P

GRID = 384
ORDER = 4
SPLITTING = 0.8
AXES = ("gz", "gy")
RADIX = 3


def round_up(value, unit):
    return -(-value // unit) * unit


def window_start(z_part, z_local):
    return pl.multiple_of(z_part * z_local // 8 * 8, 8)


def spline_weights(frac):
    remain = 1.0 - frac
    square = frac * frac
    cubed = square * frac
    values = [
        remain * remain * remain / 6.0,
        (3.0 * cubed - 6.0 * square + 4.0) / 6.0,
        (-3.0 * cubed + 3.0 * square + 3.0 * frac + 1.0) / 6.0,
        cubed / 6.0,
    ]
    slopes = [
        -0.5 * remain * remain,
        (3.0 * square - 4.0 * frac) / 2.0,
        (-3.0 * square + 2.0 * frac + 1.0) / 2.0,
        0.5 * square,
    ]
    return values, slopes


def sine_of_turns(turn):
    square = turn * turn
    total = jnp.full_like(turn, 0.0)
    for power in range(6, -1, -1):
        term = (-1.0) ** power * (2.0 * math.pi) ** (2 * power + 1) / math.factorial(2 * power + 1)
        total = total * square + term
    return total * turn


def cos_sin_of_turns(turn):
    folded = jnp.minimum(jnp.maximum(turn, -0.5 - turn), 0.5 - turn)
    return sine_of_turns(0.25 - jnp.abs(turn)), sine_of_turns(folded)


def halves(value):
    high = value.astype(jnp.bfloat16)
    low = (value - high.astype(jnp.float32)).astype(jnp.bfloat16)
    return high, low


def dot(left, right, contract=((1,), (0,))):
    return lax.dot_general(left, right, (contract, ((), ())), preferred_element_type=jnp.float32)


def x_phases(cells, kx_column, points):
    product = kx_column * cells
    turn = product * (1.0 / points)
    rest = product - points * jnp.floor(turn + 0.5)
    return cos_sin_of_turns(rest * (1.0 / points))


def spread_kernel(
    place_ref, kx_ref, *refs, count, points, z_local, y_local, kx_here, z_rows, y_rows, chunk, opening
):
    blocks = refs[:count]
    out_ref, phase_ref, slots, arrived = refs[-4:]
    step = pl.program_id(0)
    z_part = place_ref[step, 0]
    y_part = place_ref[step, 1]
    atoms = slots.shape[2]
    cells = ORDER**3
    parts = 2 * kx_here

    def fetch(n):
        return pltpu.make_async_copy(blocks[n], slots.at[n % 2], arrived.at[n % 2])

    @pl.when(step == 0)
    def _():
        fetch(0).start()
        if opening:
            out_ref[...] = jnp.zeros_like(out_ref)

    for n in range(1, count):

        @pl.when(step + 1 == n)
        def _():
            fetch(n).start()

    slot = step % 2
    pltpu.make_async_copy(blocks[0], slots.at[slot], arrived.at[slot]).wait()
    rec_ref = slots.at[pl.ds(slot, 1)]

    start = window_start(z_part, z_local)
    first_z = start.astype(jnp.float32)
    first_y = (y_part * y_local).astype(jnp.float32)
    base_cos, base_sin = x_phases(rec_ref[0, cells + 2 : cells + 3, :], kx_ref[:, 0:1], points)
    phase_ref[0, :kx_here, :] = base_cos
    phase_ref[0, kx_here:, :] = -base_sin
    for c in range(1, ORDER):
        turn_cos = kx_ref[:, 2 * c : 2 * c + 1]
        turn_sin = kx_ref[:, 2 * c + 1 : 2 * c + 2]
        phase_ref[c, :kx_here, :] = base_cos * turn_cos - base_sin * turn_sin
        phase_ref[c, kx_here:, :] = -(base_sin * turn_cos + base_cos * turn_sin)
    groups = z_rows // 8
    sums = [None] * ORDER
    for first in range(0, atoms, chunk):
        span = slice(first, first + chunk)
        local_z = (rec_ref[0, cells : cells + 1, span] - first_z).astype(jnp.int32)
        local_y = (rec_ref[0, cells + 1 : cells + 2, span] - first_y).astype(jnp.int32)
        offset_z = lax.broadcasted_iota(jnp.int32, (8, chunk), 0) - local_z
        offset_y = lax.broadcasted_iota(jnp.int32, (y_rows, chunk), 0) - local_y
        hits = jnp.where(offset_y == 0, 1.0, 0.0).astype(jnp.bfloat16)
        masks = []
        for m in range(groups):
            inside = jnp.where(((offset_z + 8 * m) & (-ORDER)) == 0, 1.0, 0.0)
            masks.append(jnp.concatenate([inside, inside], axis=0).astype(jnp.bfloat16)[None])
        for b in range(ORDER):
            weights = []
            for c in range(ORDER):
                row = (b * ORDER + c) * ORDER
                four = rec_ref[0, row : row + ORDER, span]
                weights.append(jnp.concatenate([four] * (8 // ORDER), axis=0))
            lines = []
            for n in range(parts):
                line = weights[0] * phase_ref[0, n : n + 1, span]
                for c in range(1, ORDER):
                    line = line + weights[c] * phase_ref[c, n : n + 1, span]
                lines.append(line)
            for piece in halves(jnp.concatenate(lines, axis=0)):
                tiles = piece.reshape(kx_here, 16, chunk)
                stacked = jnp.concatenate(
                    [(tiles * mask).reshape(16 * kx_here, chunk) for mask in masks], axis=0
                )
                product = dot(stacked, hits, ((1,), (1,)))
                sums[b] = product if sums[b] is None else sums[b] + product
    total = sums[0]
    for b in range(1, ORDER):
        total = total + pltpu.roll(sums[b], b, 1)
    for m in range(groups):
        for n in range(parts):
            row = (m * parts + n) * 8
            out_ref[y_part, n, pl.ds(start + 8 * m, 8), :] += total[row : row + 8]


def split_dot(value, high, low):
    top, rest = halves(value)
    return dot(top, high) + (dot(rest, high) + dot(top, low))


def split_dot_left(high, low, value):
    top, rest = halves(value)
    return dot(high, top) + (dot(high, rest) + dot(low, top))


HALF_ROOT = math.sqrt(3.0) / 2.0


def three_way(parts, sign):
    (ar, ai), (br, bi), (cr, ci) = parts
    sum_r, sum_i = br + cr, bi + ci
    dif_r, dif_i = (br - cr) * HALF_ROOT, (bi - ci) * HALF_ROOT
    mid_r, mid_i = ar - 0.5 * sum_r, ai - 0.5 * sum_i
    return [
        (ar + sum_r, ai + sum_i),
        (mid_r - sign * dif_i, mid_i + sign * dif_r),
        (mid_r + sign * dif_i, mid_i - sign * dif_r),
    ]


def turned(value, cosine, sine, sign):
    re, im = value
    return (re * cosine - sign * (im * sine), im * cosine + sign * (re * sine))


def transform_kernel(
    scal_ref, re_ref, im_ref, right_hi, right_lo, left_hi, left_lo, tw_row, tw_col, row_ref, col_ref,
    out_ref, *, points, y_local, count_y, third,
):
    index = pl.program_id(0)
    z_pad = re_ref.shape[2]
    y_rows = re_ref.shape[3]

    def whole(ref):
        plane = None
        for q in range(count_y):
            piece = ref[q, 0]
            body = piece[:points]
            spare = z_pad - points
            body = jnp.concatenate([body[:spare] + piece[points:], body[spare:]], axis=0)
            if y_rows < points:
                body = jnp.concatenate(
                    [body, jnp.zeros((points, points - y_rows), jnp.float32)], axis=1
                )
            if q > 0:
                body = pltpu.roll(body, q * y_local, 1)
            plane = body if plane is None else plane + body
        return plane

    def lanes(value, part):
        return tuple(v[:, part * third : (part + 1) * third] for v in value)

    def rows(value, part):
        return tuple(v[part * third : (part + 1) * third] for v in value)

    plane = (whole(re_ref), whole(im_ref))
    parts = three_way([lanes(plane, n) for n in range(RADIX)], -1.0)
    done = []
    for n, part in enumerate(parts):
        if n > 0:
            part = turned(part, tw_row[2 * n : 2 * n + 1, :], tw_row[2 * n + 1 : 2 * n + 2, :], -1.0)
        done.append(split_dot(jnp.concatenate(part, axis=1), right_hi[...], right_lo[...]))
    parts = three_way(
        [
            (
                jnp.concatenate([d[n * third : (n + 1) * third, :third] for d in done], axis=1),
                jnp.concatenate([d[n * third : (n + 1) * third, third:] for d in done], axis=1),
            )
            for n in range(RADIX)
        ],
        -1.0,
    )
    scale = scal_ref[index, 0]
    square = scal_ref[index, 1]
    back = []
    for n, part in enumerate(parts):
        if n > 0:
            cosine = jnp.concatenate([tw_col[2 * n]] * RADIX, axis=1)
            sine = jnp.concatenate([tw_col[2 * n + 1]] * RADIX, axis=1)
            part = turned(part, cosine, sine, -1.0)
        spectrum = split_dot_left(left_hi[...], left_lo[...], jnp.concatenate(part, axis=0))
        col_factor = jnp.concatenate([col_ref[0, n * third : (n + 1) * third, :]] * RADIX, axis=1)
        col_square = jnp.concatenate([col_ref[1, n * third : (n + 1) * third, :]] * RADIX, axis=1)
        total = col_square + row_ref[1:2, :] + square
        safe = jnp.where(total > 0.0, total, 1.0)
        green = jnp.where(total > 0.0, col_factor * row_ref[0:1, :] * scale / (math.pi * safe), 0.0)
        swapped = jnp.concatenate([spectrum[third:] * green, spectrum[:third] * green], axis=0)
        result = split_dot_left(left_hi[...], left_lo[...], swapped)
        part = (result[third:], result[:third])
        if n > 0:
            part = turned(part, cosine, sine, 1.0)
        back.append(part)
    back = three_way(back, 1.0)
    plane = tuple(jnp.concatenate([b[i] for b in back], axis=0) for i in range(2))
    parts = []
    for n in range(RADIX):
        re, im = lanes(plane, n)
        result = split_dot(jnp.concatenate([im, re], axis=1), right_hi[...], right_lo[...])
        part = (result[:, third:], result[:, :third])
        if n > 0:
            part = turned(part, tw_row[2 * n : 2 * n + 1, :], tw_row[2 * n + 1 : 2 * n + 2, :], 1.0)
        parts.append(part)
    parts = three_way(parts, 1.0)
    spare = out_ref.shape[2] - points
    for i in range(2):
        value = jnp.concatenate([p[i] for p in parts], axis=1)
        out_ref[i, 0, :points, :] = value
        out_ref[i, 0, points:, :] = value[:spare]


def force_kernel(
    where_ref, kx_ref, *refs, points, z_local, kx_here, z_rows, count_y
):
    del where_ref
    qm_refs, (pot_ref, out_ref) = refs[:count_y], refs[count_y:]
    z_part = pl.program_id(0)
    start = window_start(z_part, z_local)
    first_z = start.astype(jnp.float32)
    window = jnp.concatenate(
        [pot_ref[i, k, pl.ds(start, z_rows), :] for i in range(2) for k in range(kx_here)], axis=0
    )
    top, rest = halves(window)

    def placed(offset, weights):
        value = jnp.zeros(offset.shape, jnp.float32)
        for a in range(ORDER):
            value = jnp.where(offset == a, weights[a], value)
        return value

    for q in range(count_y):
        qm_ref = qm_refs[q]
        atoms = qm_ref.shape[2]
        local_z = (qm_ref[0, 0:1, :] - first_z).astype(jnp.int32)
        cell_y = qm_ref[0, 1:2, :].astype(jnp.int32)
        w_z, d_z = spline_weights(qm_ref[0, 3:4, :])
        w_y, d_y = spline_weights(qm_ref[0, 4:5, :])
        w_x, d_x = spline_weights(qm_ref[0, 5:6, :])
        offset_z = lax.broadcasted_iota(jnp.int32, (z_rows, atoms), 0) - local_z
        plane_w, plane_d = placed(offset_z, w_z)[None], placed(offset_z, d_z)[None]
        offset_y = lax.broadcasted_iota(jnp.int32, (points, atoms), 0) - cell_y
        offset_y = jnp.where(offset_y < 0, offset_y + points, offset_y)
        row_hi, row_lo = halves(jnp.concatenate([placed(offset_y, w_y), placed(offset_y, d_y)], axis=1))
        along = dot(top, row_hi) + (dot(rest, row_hi) + dot(top, row_lo))
        along = along.reshape(2 * kx_here, z_rows, 2 * atoms)
        sum_z = jnp.sum(along[:, :, :atoms] * plane_d, axis=1)
        sum_y = jnp.sum(along[:, :, atoms:] * plane_w, axis=1)
        sum_x = jnp.sum(along[:, :, :atoms] * plane_w, axis=1)
        base_cos, base_sin = x_phases(qm_ref[0, 2:3, :], kx_ref[:, 0:1], points)
        line_w = [w_x[0] * base_cos, w_x[0] * base_sin]
        line_d = [d_x[0] * base_cos, d_x[0] * base_sin]
        for c in range(1, ORDER):
            turn_cos = kx_ref[:, 2 * c : 2 * c + 1]
            turn_sin = kx_ref[:, 2 * c + 1 : 2 * c + 2]
            cosine = base_cos * turn_cos - base_sin * turn_sin
            sine = base_sin * turn_cos + base_cos * turn_sin
            line_w = [line_w[0] + w_x[c] * cosine, line_w[1] + w_x[c] * sine]
            line_d = [line_d[0] + d_x[c] * cosine, line_d[1] + d_x[c] * sine]
        line_w = jnp.concatenate([line_w[0], -line_w[1]], axis=0)
        line_d = jnp.concatenate([line_d[0], -line_d[1]], axis=0)
        out_ref[q, 0:1, :] = jnp.sum(sum_z * line_w, axis=0, keepdims=True)
        out_ref[q, 1:2, :] = jnp.sum(sum_y * line_w, axis=0, keepdims=True)
        out_ref[q, 2:3, :] = jnp.sum(sum_x * line_d, axis=0, keepdims=True)


def tables(points):
    third = points // RADIX
    index = np.arange(third)
    angle = 2.0 * np.pi / third * (np.outer(index, index) % third)
    cosine, sine = np.cos(angle), np.sin(angle)
    right = np.block([[cosine, -sine], [sine, cosine]])
    left = np.block([[cosine, sine], [-sine, cosine]])

    def split(matrix):
        value = jnp.asarray(matrix, jnp.float32)
        high = jnp.asarray(matrix.astype(jnp.bfloat16))
        low = jnp.asarray((matrix - matrix.astype(jnp.bfloat16).astype(np.float64)).astype(jnp.bfloat16))
        return high, low

    turn = 2.0 * np.pi / points * np.outer(np.arange(RADIX), index)
    twiddle = np.stack([np.cos(turn), np.sin(turn)], axis=1).reshape(2 * RADIX, third).astype(np.float32)
    tw_row = jnp.asarray(twiddle)
    tw_col = jnp.asarray(np.broadcast_to(twiddle[:, :, None], (2 * RADIX, third, third)).copy())
    slots = (RADIX * np.arange(third)[None, :] + np.arange(RADIX)[:, None]).reshape(-1)
    factor, square = factors(slots, points)
    row = jnp.asarray(np.stack([factor, square]).astype(np.float32))
    col = jnp.asarray(
        np.broadcast_to(np.stack([factor, square])[:, :, None], (2, points, third)).astype(np.float32)
    )
    return split(right) + split(left) + (tw_row, tw_col, row, col)


def factors(index, points):
    signed = np.where(index < points // 2, index, index - points) / points
    spline = 2.0 / 3.0 + np.cos(2.0 * np.pi * index / points) / 3.0
    factor = np.exp(-((np.pi / SPLITTING) ** 2) * signed**2) / spline**2
    return np.where(index == points // 2, 0.0, factor), signed**2


def staged(record, outer, spread):
    def index(where):
        z, x, core, y = where
        return ((z * 2 + x) * 2 + core) * 2 + y

    everyone = [(z, x, c, y) for z in range(outer) for x in range(2) for c in range(2) for y in range(2)]

    def across_x(w):
        return (w[0], 1 - w[1], w[2], w[3])

    def across_y(w):
        return (w[0], w[1], w[2], 1 - w[3])

    def partner(w):
        return (w[0], w[1], 1 - w[2], w[3])

    def chosen(core, first, second):
        return tuple(jnp.where(core == 0, f, s) if f is not s else f for f, s in zip(first, second))

    def flip_one(w):
        if isinstance(w[2], int):
            return across_x(w) if w[2] == 0 else across_y(w)
        return chosen(w[2], across_x(w), across_y(w))

    def flip_two(w):
        if isinstance(w[2], int):
            return across_y(w) if w[2] == 0 else across_x(w)
        return chosen(w[2], across_y(w), across_x(w))

    gz, gy = lax.axis_index("gz"), lax.axis_index("gy")
    own = (gz // 4, gz // 2 % 2, gz % 2, gy)

    def moved(block, sender):
        array, source = block
        route = [(index(sender(w)), index(w)) for w in everyone]
        return lax.ppermute(array, AXES, route), lambda w: source(sender(w))

    def after(planes, blocks):
        arrays, planes = lax.optimization_barrier(([b[0] for b in blocks], planes))
        return planes, [(array, b[1]) for array, b in zip(arrays, blocks)]

    def add(planes, blocks):
        ready = []
        for array, source in blocks:
            z, x, core, y = source(own)
            ready.append((array, (z * 2 + x) * 2 + core, y))
        return spread(planes, ready)

    def each(blocks, sender):
        return [moved(block, sender) for block in blocks]

    mine = (record, lambda w: w)
    shift = [
        moved(mine, lambda w, n=n: ((w[0] - n) % outer, w[1], w[2], w[3])) for n in range(1, outer)
    ]
    near = [moved(mine, flip_one), moved(mine, flip_two)]
    other = [moved(mine, partner)]
    planes = add(None, [mine])
    planes = add(planes, other)
    planes, near = after(planes, near)
    near_partner = each(near, partner)
    far = each(near[:1], flip_two)
    planes = add(planes, near)
    planes = add(planes, near_partner)
    planes, held = after(planes, shift + far)
    shift, far = held[:-1], held[-1:]
    one, two = each(shift, flip_one), each(shift, flip_two)
    shift_partner = each(shift, partner)
    far_partner = each(far, partner)
    planes = add(planes, far + shift)
    planes = add(planes, far_partner + shift_partner)
    planes, held = after(planes, one + two)
    one, two = held[: len(one)], held[len(one) :]
    both = each(one, flip_two)
    one_partner, two_partner = each(one, partner), each(two, partner)
    planes = add(planes, one + two)
    planes, both = after(planes, both)
    both_partner = each(both, partner)
    planes = add(planes, one_partner + two_partner)
    return add(planes, both + both_partner)


def shards(spread_weights, spread_base, qm_base, qm_frac, qm_charge):
    points = GRID
    count_z = lax.axis_size("gz")
    count_y = lax.axis_size("gy")
    devices = count_z * count_y
    z_local = points // count_z
    y_local = points // count_y
    kx_here = -(-(points // 2) // devices)
    here = lax.axis_index("gz") * count_y + lax.axis_index("gy")
    kx = here * kx_here + jnp.arange(kx_here, dtype=jnp.int32)
    z_rows = round_up(z_local + ORDER - 1 + (0 if z_local % 8 == 0 else 7), 8)
    z_pad = (points - z_local) // 8 * 8 + z_rows
    y_rows = min(round_up(y_local + ORDER - 1, 128), points)

    atoms = spread_weights.shape[1]
    qms = qm_charge.shape[0]
    qm_rows = jnp.concatenate([qm_base.astype(jnp.float32), qm_frac], axis=0).reshape(-1)
    lines = -(-qm_rows.shape[0] // atoms)
    qm_rows = jnp.pad(qm_rows, (0, lines * atoms - qm_rows.shape[0])).reshape(lines, atoms)
    by_plane = spread_weights.reshape(ORDER, ORDER * ORDER, 1, atoms)
    plane = (jnp.arange(ORDER)[:, None] - spread_base[0][None, :]) % ORDER
    placed = jnp.zeros((ORDER * ORDER, ORDER, atoms), jnp.float32)
    for a in range(ORDER):
        placed = jnp.where(plane[None] == a, by_plane[a], placed)
    placed = placed.reshape(ORDER**3, atoms)
    record = jnp.concatenate([placed, spread_base.astype(jnp.float32), qm_rows], axis=0)
    held = round_up(record.shape[0], 8)
    record = jnp.pad(record, ((0, held - record.shape[0]), (0, 0)))
    fkx = kx.astype(jnp.float32)
    turn = 2.0 * math.pi / points * ((kx[:, None] * jnp.arange(ORDER)[None, :]) % points).astype(jnp.float32)
    kx_table = jnp.stack([jnp.cos(turn), jnp.sin(turn)], axis=2).reshape(kx_here, 2 * ORDER)
    kx_table = kx_table.at[:, 0].set(fkx)

    planes = (count_y, 2 * kx_here, z_pad, y_rows)
    first_line = ORDER**3 + 3
    seen = []

    def spread(held_planes, blocks):
        place = jnp.stack([jnp.stack([block[1], block[2]]) for block in blocks])
        seen.extend((block[0][first_line : first_line + lines], block[1] * count_y + block[2]) for block in blocks)
        opening = held_planes is None
        count = len(blocks)
        hbm = pl.BlockSpec(memory_space=pltpu.HBM)
        vmem = pl.BlockSpec(memory_space=pltpu.VMEM)
        return pl.pallas_call(
            lambda *refs: spread_kernel(
                *refs, count=count, points=points, z_local=z_local, y_local=y_local,
                kx_here=kx_here, z_rows=z_rows, y_rows=y_rows, chunk=math.gcd(atoms, 256),
                opening=opening,
            ),
            grid=(count,),
            in_specs=[
                pl.BlockSpec(memory_space=pltpu.SMEM),
                pl.BlockSpec(kx_table.shape, lambda d: (0, 0)),
            ]
            + [hbm] * count
            + ([] if opening else [vmem]),
            out_specs=vmem,
            out_shape=pltpu.VMEM(planes, jnp.float32),
            scratch_shapes=[
                pltpu.VMEM((ORDER, 2 * kx_here, atoms), jnp.float32),
                pltpu.VMEM((2, held, atoms), jnp.float32),
                pltpu.SemaphoreType.DMA((2,)),
            ],
            input_output_aliases={} if opening else {2 + count: 0},
            compiler_params=pltpu.CompilerParams(
                dimension_semantics=("arbitrary",), vmem_limit_bytes=24 * 1024 * 1024
            ),
            cost_estimate=pl.CostEstimate(
                flops=count * atoms * ORDER * parts_flops, bytes_accessed=0, transcendentals=0
            ),
            name="spread",
        )(place, kx_table, *[block[0] for block in blocks], *([] if opening else [held_planes]))

    parts_flops = 4 * z_rows * 2 * kx_here * y_rows
    if count_y == 2 and count_z % 4 == 0:
        spread_planes = staged(record, count_z // 4, spread)
    else:
        records = lax.all_gather(record, AXES, axis=0, tiled=False)
        spread_planes = None
        for first in range(0, devices, 32):
            blocks = [
                (records[d], jnp.int32(d // count_y), jnp.int32(d % count_y))
                for d in range(first, min(first + 32, devices))
            ]
            spread_planes = spread(spread_planes, blocks)

    signed = fkx / points
    spline = 2.0 / 3.0 + jnp.cos(2.0 * math.pi / points * fkx) / 3.0
    kx_factor = jnp.exp(-((math.pi / SPLITTING) ** 2) * signed * signed) / (spline * spline)
    kx_factor = kx_factor * jnp.where(kx == 0, 1.0, 2.0) / float(points) ** 3
    kx_factor = jnp.where(kx < points // 2, kx_factor, 0.0)
    scalars = jnp.stack([kx_factor, signed * signed], axis=1)
    constants = tables(points)
    third = points // RADIX

    def fixed(array):
        return pl.BlockSpec(array.shape, lambda k, n=array.ndim: (0,) * n)

    block = (count_y, 1, z_pad, y_rows)
    potential = pl.pallas_call(
        lambda *refs: transform_kernel(
            *refs, points=points, y_local=y_local, count_y=count_y, third=third
        ),
        grid=(kx_here,),
        in_specs=[
            pl.BlockSpec(memory_space=pltpu.SMEM),
            pl.BlockSpec(block, lambda k: (0, k, 0, 0)),
            pl.BlockSpec(block, lambda k: (0, k + kx_here, 0, 0)),
        ]
        + [fixed(array) for array in constants],
        out_specs=pl.BlockSpec((2, 1, z_pad, points), lambda k: (0, k, 0, 0)),
        out_shape=jax.ShapeDtypeStruct((2, kx_here, z_pad, points), jnp.float32),
        compiler_params=pltpu.CompilerParams(
            dimension_semantics=("arbitrary",), vmem_limit_bytes=60 * 1024 * 1024
        ),
        name="transform",
    )(scalars, spread_planes, spread_planes, *constants)

    qm_all = jnp.stack([rows for rows, _ in seen]).reshape(devices, lines * atoms)
    qm_all = qm_all[:, : 6 * qms].reshape(devices, 6, qms)
    owner = jnp.stack([device for _, device in seen])
    match = owner[None, :] == jnp.arange(devices, dtype=jnp.int32)[:, None]
    where = jnp.sum(jnp.where(match, jnp.arange(devices, dtype=jnp.int32)[None, :], 0), axis=1)
    partial = pl.pallas_call(
        lambda *refs: force_kernel(
            *refs, points=points, z_local=z_local, count_y=count_y, kx_here=kx_here, z_rows=z_rows
        ),
        grid_spec=pltpu.PrefetchScalarGridSpec(
            num_scalar_prefetch=1,
            grid=(count_z,),
            in_specs=[pl.BlockSpec(kx_table.shape, lambda p, where: (0, 0))]
            + [
                pl.BlockSpec((1, 6, qms), lambda p, where, q=q: (where[p * count_y + q], 0, 0))
                for q in range(count_y)
            ]
            + [pl.BlockSpec((2, kx_here, z_pad, points), lambda p, where: (0, 0, 0, 0))],
            out_specs=pl.BlockSpec((count_y, 3, qms), lambda p, where: (p, 0, 0)),
        ),
        out_shape=jax.ShapeDtypeStruct((devices, 3, qms), jnp.float32),
        compiler_params=pltpu.CompilerParams(
            dimension_semantics=("arbitrary",), vmem_limit_bytes=40 * 1024 * 1024
        ),
        name="forces",
    )(where, kx_table, *[qm_all] * count_y, potential)
    moved = lax.all_to_all(partial, AXES, split_axis=0, concat_axis=0, tiled=True)
    return -qm_charge[None, :] * jnp.sum(moved, axis=0)


def solution(mesh):
    in_specs = (
        P(None, AXES),
        P(None, AXES),
        P(None, AXES),
        P(None, AXES),
        P(AXES),
    )
    out_specs = P(None, AXES)
    return jax.shard_map(shards, mesh=mesh, in_specs=in_specs, out_specs=out_specs, check_vma=False)
```

```python
import math

import jax
import jax.numpy as jnp
import numpy as np
from jax import lax
from jax.experimental import pallas as pl
from jax.experimental.pallas import tpu as pltpu
from jax.sharding import PartitionSpec as P

GRID = 384
ORDER = 4
SPLITTING = 0.8
AXES = ("gz", "gy")
RADIX = 3
VMEM_BYTES = 24 * 1024 * 1024


def round_up(value, unit):
    return -(-value // unit) * unit


def window_start(z_part, z_local):
    return pl.multiple_of(z_part * z_local // 8 * 8, 8)


def spline_weights(frac):
    remain = 1.0 - frac
    square = frac * frac
    cubed = square * frac
    values = [
        remain * remain * remain / 6.0,
        (3.0 * cubed - 6.0 * square + 4.0) / 6.0,
        (-3.0 * cubed + 3.0 * square + 3.0 * frac + 1.0) / 6.0,
        cubed / 6.0,
    ]
    slopes = [
        -0.5 * remain * remain,
        (3.0 * square - 4.0 * frac) / 2.0,
        (-3.0 * square + 2.0 * frac + 1.0) / 2.0,
        0.5 * square,
    ]
    return values, slopes


def sine_of_turns(turn):
    square = turn * turn
    total = jnp.full_like(turn, 0.0)
    for power in range(6, -1, -1):
        term = (-1.0) ** power * (2.0 * math.pi) ** (2 * power + 1) / math.factorial(2 * power + 1)
        total = total * square + term
    return total * turn


def cos_sin_of_turns(turn):
    folded = jnp.minimum(jnp.maximum(turn, -0.5 - turn), 0.5 - turn)
    return sine_of_turns(0.25 - jnp.abs(turn)), sine_of_turns(folded)


def halves(value):
    high = value.astype(jnp.bfloat16)
    low = (value - high.astype(jnp.float32)).astype(jnp.bfloat16)
    return high, low


def dot(left, right, contract=((1,), (0,))):
    return lax.dot_general(left, right, (contract, ((), ())), preferred_element_type=jnp.float32)


def x_phases(cells, kx_column, points):
    product = kx_column * cells
    turn = product * (1.0 / points)
    rest = product - points * jnp.floor(turn + 0.5)
    return cos_sin_of_turns(rest * (1.0 / points))


def spread_kernel(
    here_ref, place_ref, kx_ref, *refs, pieces, origin, listed, points, z_local, y_local, count_y, kx_here, z_need,
    y_rows, chunk, opening
):
    out_ref, qm_ref, phase_ref, slots, arrived = refs[-5:]
    step = pl.program_id(0)
    entry = 2 * (here_ref[0] * listed + origin + step)
    z_part = place_ref[entry]
    y_part = place_ref[entry + 1]
    held, atoms = slots.shape[1:]
    cells = ORDER**3
    parts = 2 * kx_here
    count = len(pieces)

    def fetch(n):
        array, block = pieces[n]
        source = refs[array].at[pl.ds(block * held, held)]
        return pltpu.make_async_copy(source, slots.at[n % 2], arrived.at[n % 2])

    @pl.when(step == 0)
    def _():
        fetch(0).start()
        if opening:
            out_ref[...] = jnp.zeros_like(out_ref)

    for n in range(1, count):

        @pl.when(step + 1 == n)
        def _():
            fetch(n).start()

    slot = step % 2
    pltpu.make_async_copy(refs[0].at[pl.ds(0, held)], slots.at[slot], arrived.at[slot]).wait()
    rec_ref = slots.at[slot]

    qms = qm_ref.shape[2]
    for n in range(6):
        line, lane = divmod(n * qms, atoms)
        line += cells + 3
        qm_ref[z_part * count_y + y_part, n : n + 1, :] = rec_ref[line : line + 1, lane : lane + qms]

    start = window_start(z_part, z_local)
    first_z = start.astype(jnp.float32)
    first_y = (y_part * y_local).astype(jnp.float32)
    short = kx_here % 2 == 0 and 0 < z_need % 8 <= 4
    groups = z_need // 8 if short else -(-z_need // 8)
    low_half = lax.broadcasted_iota(jnp.int32, (8, chunk), 0) < 4
    total = None
    for first in range(0, atoms, chunk):
        span = slice(first, first + chunk)
        base_cos, base_sin = x_phases(rec_ref[cells + 2 : cells + 3, span], kx_ref[:, 0:1], points)
        phase_ref[0, :kx_here, span] = base_cos
        phase_ref[0, kx_here:, span] = -base_sin
        for c in range(1, ORDER):
            turn_cos = kx_ref[:, 2 * c : 2 * c + 1]
            turn_sin = kx_ref[:, 2 * c + 1 : 2 * c + 2]
            phase_ref[c, :kx_here, span] = base_cos * turn_cos - base_sin * turn_sin
            phase_ref[c, kx_here:, span] = -(base_sin * turn_cos + base_cos * turn_sin)
        local_z = (rec_ref[cells : cells + 1, span] - first_z).astype(jnp.int32)
        local_y = (rec_ref[cells + 1 : cells + 2, span] - first_y).astype(jnp.int32)
        row = lax.broadcasted_iota(jnp.int32, (8, chunk), 0)
        offset_y = lax.broadcasted_iota(jnp.int32, (y_rows, chunk), 0) - local_y

        def mask(planes):
            inside = jnp.where(((planes - local_z) & (-ORDER)) == 0, 1.0, 0.0)
            return jnp.concatenate([inside, inside], axis=0).astype(jnp.bfloat16)[None]

        masks = [mask(row + 8 * m) for m in range(groups)]
        last = mask((row & 3) + 8 * groups) if short else None
        for b in range(ORDER):
            hits = jnp.where(offset_y == b, 1.0, 0.0).astype(jnp.bfloat16)
            weights = []
            for c in range(ORDER):
                place = (b * ORDER + c) * ORDER
                four = rec_ref[place : place + ORDER, span]
                weights.append(jnp.concatenate([four] * (8 // ORDER), axis=0))
            lines = []
            for n in range(parts):
                line = weights[0] * phase_ref[0, n : n + 1, span]
                for c in range(1, ORDER):
                    line = line + weights[c] * phase_ref[c, n : n + 1, span]
                lines.append(line)
            full = halves(jnp.concatenate(lines, axis=0))
            if short:
                pairs = [jnp.where(low_half, lines[n], lines[n + 1]) for n in range(0, parts, 2)]
                tails = halves(jnp.concatenate(pairs, axis=0))
            for i in range(2):
                tiles = full[i].reshape(kx_here, 16, chunk)
                stacked = [(tiles * m).reshape(16 * kx_here, chunk) for m in masks]
                if short:
                    tiles = tails[i].reshape(kx_here // 2, 16, chunk)
                    stacked.append((tiles * last).reshape(8 * kx_here, chunk))
                product = dot(jnp.concatenate(stacked, axis=0), hits, ((1,), (1,)))
                total = product if total is None else total + product
    for m in range(groups):
        for n in range(parts):
            row = (m * parts + n) * 8
            out_ref[y_part, n, pl.ds(start + 8 * m, 8), :] += total[row : row + 8]
    if short:
        for n in range(0, parts, 2):
            row = groups * parts * 8 + n * 4
            rows = pl.ds(start + 8 * groups, 8)
            zero = jnp.zeros((4, y_rows), jnp.float32)
            eight = total[row : row + 8]
            out_ref[y_part, n, rows, :] += jnp.concatenate([eight[:4], zero], axis=0)
            out_ref[y_part, n + 1, rows, :] += jnp.concatenate([eight[4:], zero], axis=0)


def split_dot(value, high, low):
    top, rest = halves(value)
    return dot(top, high) + (dot(rest, high) + dot(top, low))


def split_dot_left(high, low, value):
    top, rest = halves(value)
    return dot(high, top) + (dot(high, rest) + dot(low, top))


HALF_ROOT = math.sqrt(3.0) / 2.0


def three_way(parts, sign):
    (ar, ai), (br, bi), (cr, ci) = parts
    sum_r, sum_i = br + cr, bi + ci
    dif_r, dif_i = (br - cr) * HALF_ROOT, (bi - ci) * HALF_ROOT
    mid_r, mid_i = ar - 0.5 * sum_r, ai - 0.5 * sum_i
    return [
        (ar + sum_r, ai + sum_i),
        (mid_r - sign * dif_i, mid_i + sign * dif_r),
        (mid_r + sign * dif_i, mid_i - sign * dif_r),
    ]


def turned(value, cosine, sine, sign):
    re, im = value
    return (re * cosine - sign * (im * sine), im * cosine + sign * (re * sine))


def transform_kernel(
    here_ref, scal_ref, right_hi, right_lo, left_hi, left_lo, tw_row, tw_col, row_ref, col_ref,
    _, planes_ref, *, points, y_local, count_y, kx_here, third,
):
    index = pl.program_id(0)
    z_pad, y_rows = planes_ref.shape[2:]
    spare = z_pad - points

    def whole(part, n):
        line = None
        for q in range(count_y):
            body = planes_ref[q, part, n * third : (n + 1) * third, :]
            if n == 0:
                wrapped = planes_ref[q, part, points:, :]
                body = jnp.concatenate([body[:spare] + wrapped, body[spare:]], axis=0)
            if y_rows < points:
                body = jnp.concatenate(
                    [body, jnp.zeros((third, points - y_rows), jnp.float32)], axis=1
                )
            if q > 0:
                body = pltpu.roll(body, q * y_local, 1)
            line = body if line is None else line + body
        return line

    def lanes(value, part):
        return tuple(v[:, part * third : (part + 1) * third] for v in value)

    def row_turn(part, n, sign):
        if n == 0:
            return part
        return turned(part, tw_row[2 * n : 2 * n + 1, :], tw_row[2 * n + 1 : 2 * n + 2, :], sign)

    done = []
    for n in range(RADIX):
        rows = (whole(index, n), whole(index + kx_here, n))
        parts = three_way([lanes(rows, m) for m in range(RADIX)], -1.0)
        pieces = []
        for m, part in enumerate(parts):
            part = row_turn(part, m, -1.0)
            pieces.append(split_dot(jnp.concatenate(part, axis=1), right_hi[...], right_lo[...]))
        done.append(
            tuple(
                jnp.concatenate([p[:, i * third : (i + 1) * third] for p in pieces], axis=1)
                for i in range(2)
            )
        )
    parts = three_way(done, -1.0)
    entry = 2 * (here_ref[0] * kx_here + index)
    scale = scal_ref[entry]
    square = scal_ref[entry + 1]
    back = []
    for n, part in enumerate(parts):
        if n > 0:
            cosine = jnp.concatenate([tw_col[2 * n]] * RADIX, axis=1)
            sine = jnp.concatenate([tw_col[2 * n + 1]] * RADIX, axis=1)
            part = turned(part, cosine, sine, -1.0)
        spectrum = split_dot_left(left_hi[...], left_lo[...], jnp.concatenate(part, axis=0))
        col_factor = jnp.concatenate([col_ref[0, n * third : (n + 1) * third, :]] * RADIX, axis=1)
        col_square = jnp.concatenate([col_ref[1, n * third : (n + 1) * third, :]] * RADIX, axis=1)
        total = col_square + row_ref[1:2, :] + square
        safe = jnp.where(total > 0.0, total, 1.0)
        green = jnp.where(total > 0.0, col_factor * row_ref[0:1, :] * scale / (math.pi * safe), 0.0)
        swapped = jnp.concatenate([spectrum[third:] * green, spectrum[:third] * green], axis=0)
        result = split_dot_left(left_hi[...], left_lo[...], swapped)
        part = (result[third:], result[:third])
        if n > 0:
            part = turned(part, cosine, sine, 1.0)
        back.append(part)
    back = three_way(back, 1.0)
    for n in range(RADIX):
        parts = []
        for m in range(RADIX):
            re, im = lanes(back[n], m)
            result = split_dot(jnp.concatenate([im, re], axis=1), right_hi[...], right_lo[...])
            parts.append(row_turn((result[:, third:], result[:, :third]), m, 1.0))
        parts = three_way(parts, 1.0)
        for i in range(2):
            value = jnp.concatenate([p[i] for p in parts], axis=1)
            for q, first in enumerate(range(0, points, y_rows)):
                part = value[:, first : first + y_rows]
                width = part.shape[1]
                held = index + i * kx_here
                planes_ref[q, held, n * third : (n + 1) * third, :width] = part
                if n == 0:
                    planes_ref[q, held, points:, :width] = part[:spare]


def force_kernel(kx_ref, qm_ref, pot_ref, out_ref, *, points, z_local, kx_here, z_rows, count_y):
    z_part = pl.program_id(0)
    atoms = qm_ref.shape[2]
    start = window_start(z_part, z_local)
    first_z = start.astype(jnp.float32)
    y_rows = pot_ref.shape[3]
    window = jnp.concatenate(
        [
            pot_ref[q, :, pl.ds(start, z_rows), : min(y_rows, points - first)].reshape(
                2 * kx_here * z_rows, -1
            )
            for q, first in enumerate(range(0, points, y_rows))
        ],
        axis=1,
    )
    top, rest = halves(window)

    def placed(offset, weights):
        value = jnp.zeros(offset.shape, jnp.float32)
        for a in range(ORDER):
            value = jnp.where(offset == a, weights[a], value)
        return value

    for q in range(count_y):
        row = z_part * count_y + q
        local_z = (qm_ref[row, 0:1, :] - first_z).astype(jnp.int32)
        cell_y = qm_ref[row, 1:2, :].astype(jnp.int32)
        w_z, d_z = spline_weights(qm_ref[row, 3:4, :])
        w_y, d_y = spline_weights(qm_ref[row, 4:5, :])
        w_x, d_x = spline_weights(qm_ref[row, 5:6, :])
        offset_z = lax.broadcasted_iota(jnp.int32, (z_rows, atoms), 0) - local_z
        plane_w, plane_d = placed(offset_z, w_z)[None], placed(offset_z, d_z)[None]
        offset_y = lax.broadcasted_iota(jnp.int32, (points, atoms), 0) - cell_y
        offset_y = jnp.where(offset_y < 0, offset_y + points, offset_y)
        row_hi, row_lo = halves(jnp.concatenate([placed(offset_y, w_y), placed(offset_y, d_y)], axis=1))
        along = dot(top, row_hi) + (dot(rest, row_hi) + dot(top, row_lo))
        along = along.reshape(2 * kx_here, z_rows, 2 * atoms)
        sum_z = jnp.sum(along[:, :, :atoms] * plane_d, axis=1)
        sum_y = jnp.sum(along[:, :, atoms:] * plane_w, axis=1)
        sum_x = jnp.sum(along[:, :, :atoms] * plane_w, axis=1)
        base_cos, base_sin = x_phases(qm_ref[row, 2:3, :], kx_ref[:, 0:1], points)
        line_w = [w_x[0] * base_cos, w_x[0] * base_sin]
        line_d = [d_x[0] * base_cos, d_x[0] * base_sin]
        for c in range(1, ORDER):
            turn_cos = kx_ref[:, 2 * c : 2 * c + 1]
            turn_sin = kx_ref[:, 2 * c + 1 : 2 * c + 2]
            cosine = base_cos * turn_cos - base_sin * turn_sin
            sine = base_sin * turn_cos + base_cos * turn_sin
            line_w = [line_w[0] + w_x[c] * cosine, line_w[1] + w_x[c] * sine]
            line_d = [line_d[0] + d_x[c] * cosine, line_d[1] + d_x[c] * sine]
        line_w = jnp.concatenate([line_w[0], -line_w[1]], axis=0)
        line_d = jnp.concatenate([line_d[0], -line_d[1]], axis=0)
        out_ref[q, 0:1, :] = jnp.sum(sum_z * line_w, axis=0, keepdims=True)
        out_ref[q, 1:2, :] = jnp.sum(sum_y * line_w, axis=0, keepdims=True)
        out_ref[q, 2:3, :] = jnp.sum(sum_x * line_d, axis=0, keepdims=True)


def tables(points):
    third = points // RADIX
    index = np.arange(third)
    angle = 2.0 * np.pi / third * (np.outer(index, index) % third)
    cosine, sine = np.cos(angle), np.sin(angle)
    right = np.block([[cosine, -sine], [sine, cosine]])
    left = np.block([[cosine, sine], [-sine, cosine]])

    def split(matrix):
        value = jnp.asarray(matrix, jnp.float32)
        high = jnp.asarray(matrix.astype(jnp.bfloat16))
        low = jnp.asarray((matrix - matrix.astype(jnp.bfloat16).astype(np.float64)).astype(jnp.bfloat16))
        return high, low

    turn = 2.0 * np.pi / points * np.outer(np.arange(RADIX), index)
    twiddle = np.stack([np.cos(turn), np.sin(turn)], axis=1).reshape(2 * RADIX, third).astype(np.float32)
    tw_row = jnp.asarray(twiddle)
    tw_col = jnp.asarray(np.broadcast_to(twiddle[:, :, None], (2 * RADIX, third, third)).copy())
    slots = (RADIX * np.arange(third)[None, :] + np.arange(RADIX)[:, None]).reshape(-1)
    factor, square = factors(slots, points)
    row = jnp.asarray(np.stack([factor, square]).astype(np.float32))
    col = jnp.asarray(
        np.broadcast_to(np.stack([factor, square])[:, :, None], (2, points, third)).astype(np.float32)
    )
    return split(right) + split(left) + (tw_row, tw_col, row, col)


def kx_tables(devices, kx_here, points):
    kx = np.arange(devices * kx_here)
    turn = 2.0 * np.pi / points * (kx[:, None] * np.arange(ORDER)[None, :] % points)
    columns = np.stack([np.cos(turn), np.sin(turn)], axis=2).reshape(-1, 2 * ORDER)
    columns[:, 0] = kx
    factor, square = factors(kx, points)
    factor = np.where(kx < points // 2, factor, 0.0) * np.where(kx == 0, 1.0, 2.0) / float(points) ** 3
    scalars = np.stack([factor, square], axis=1)
    shape = (devices, kx_here, -1)
    return columns.reshape(shape).astype(np.float32), scalars.reshape(shape).astype(np.float32)


def factors(index, points):
    signed = np.where(index < points // 2, index, index - points) / points
    spline = 2.0 / 3.0 + np.cos(2.0 * np.pi * index / points) / 3.0
    factor = np.exp(-((np.pi / SPLITTING) ** 2) * signed**2) / spline**2
    return np.where(index == points // 2, 0.0, factor), signed**2


def staged(record, outer, spread):
    def index(where):
        z, x, core, y = where
        return ((z * 2 + x) * 2 + core) * 2 + y

    everyone = [(z, x, c, y) for z in range(outer) for x in range(2) for c in range(2) for y in range(2)]

    def across(w, over_x):
        return (w[0], 1 - w[1], w[2], w[3]) if over_x else (w[0], w[1], w[2], 1 - w[3])

    def flip_one(w):
        return across(w, w[2] == 0)

    def flip_two(w):
        return across(w, w[2] == 1)

    def partner(w):
        return (w[0], w[1], 1 - w[2], w[3])

    def moved(batch, sender):
        array, sources = batch
        route = [(index(sender(w)), index(w)) for w in everyone]
        return lax.ppermute(array, AXES, route), [lambda w, s=s: s(sender(w)) for s in sources]

    def after(state, batches):
        arrays, state = lax.optimization_barrier(([b[0] for b in batches], state))
        return state, [(array, b[1]) for array, b in zip(arrays, batches)]

    def together(batches):
        return jnp.concatenate([b[0] for b in batches], axis=0), [s for b in batches for s in b[1]]

    mine = (record, [lambda w: w])
    shift = [
        moved(mine, lambda w, n=n: ((w[0] - n) % outer, w[1], w[2], w[3])) for n in range(1, outer)
    ]
    other = moved(mine, partner)
    one, two = moved(mine, flip_one), moved(mine, flip_two)

    def names(sources, sender=lambda w: w):
        return [lambda w, s=s: s(sender(w)) for s in sources]

    def chain(*senders):
        def source(w):
            for sender in senders:
                w = sender(w)
            return w

        return source

    shifts = [s for batch in shift for s in batch[1]]
    listed = (
        [lambda w: w, partner, flip_one, flip_two, chain(partner, flip_one), chain(partner, flip_two)]
        + [chain(flip_two, flip_one)] + shifts
        + [chain(partner, flip_two, flip_one)] + names(shifts, partner)
        + names(shifts, flip_one) + names(shifts, flip_two)
        + names(shifts, chain(partner, flip_one)) + names(shifts, chain(partner, flip_two))
        + names(shifts, chain(flip_two, flip_one)) + names(shifts, chain(partner, flip_two, flip_one))
    )
    parts = [[(index(s(w)) // 2, index(s(w)) % 2) for s in listed] for w in everyone]
    assert all(len(set(row)) == len(everyone) for row in parts)
    place = jnp.asarray(np.asarray(parts, np.int32).reshape(-1))
    origin = 0

    def add(state, batches):
        nonlocal origin
        first = origin
        for _, sources in batches:
            for source in sources:
                assert all(source(w) == listed[origin](w) for w in everyone)
                origin += 1
        return spread(state, [batch[0] for batch in batches], place, len(listed), first)

    state = add(None, [mine, other])
    state, (one, two) = after(state, [one, two])
    both = moved(one, flip_two)
    one_partner, two_partner = moved(one, partner), moved(two, partner)
    state = add(state, [one, two])
    state = add(state, [one_partner, two_partner])
    state, (both, *shift) = after(state, [both] + shift)
    shift = together(shift)
    shift_one, shift_two = moved(shift, flip_one), moved(shift, flip_two)
    both_partner, shift_partner = moved(both, partner), moved(shift, partner)
    state = add(state, [both, shift])
    state = add(state, [both_partner, shift_partner])
    state, (shift_one, shift_two) = after(state, [shift_one, shift_two])
    shift_both = moved(shift_one, flip_two)
    one_partner, two_partner = moved(shift_one, partner), moved(shift_two, partner)
    state = add(state, [shift_one, shift_two])
    state, (shift_both,) = after(state, [shift_both])
    both_partner = moved(shift_both, partner)
    state = add(state, [one_partner, two_partner])
    return add(state, [shift_both, both_partner])


def shards(spread_weights, spread_base, qm_base, qm_frac, qm_charge):
    points = GRID
    count_z = lax.axis_size("gz")
    count_y = lax.axis_size("gy")
    devices = count_z * count_y
    z_local = points // count_z
    y_local = points // count_y
    kx_here = -(-(points // 2) // devices)
    here = lax.axis_index("gz") * count_y + lax.axis_index("gy")
    z_rows = round_up(z_local + ORDER - 1 + (0 if z_local % 8 == 0 else 7), 8)
    z_pad = (points - z_local) // 8 * 8 + z_rows
    y_rows = min(round_up(y_local + ORDER - 1, 128), points)

    atoms = spread_weights.shape[1]
    qms = qm_charge.shape[0]
    qm_rows = jnp.concatenate([qm_base.astype(jnp.float32), qm_frac], axis=0).reshape(-1)
    lines = -(-qm_rows.shape[0] // atoms)
    qm_rows = jnp.pad(qm_rows, (0, lines * atoms - qm_rows.shape[0])).reshape(lines, atoms)
    by_plane = spread_weights.reshape(ORDER, ORDER * ORDER, 1, atoms)
    plane = (jnp.arange(ORDER)[:, None] - spread_base[0][None, :]) % ORDER
    placed = jnp.zeros((ORDER * ORDER, ORDER, atoms), jnp.float32)
    for a in range(ORDER):
        placed = jnp.where(plane[None] == a, by_plane[a], placed)
    placed = placed.reshape(ORDER**3, atoms)
    record = jnp.concatenate([placed, spread_base.astype(jnp.float32), qm_rows], axis=0)
    held = round_up(record.shape[0], 8)
    record = jnp.pad(record, ((0, held - record.shape[0]), (0, 0)))
    kx_columns, kx_scalars = kx_tables(devices, kx_here, points)
    here_row = here.astype(jnp.int32).reshape(1)
    kx_table = lax.dynamic_index_in_dim(jnp.asarray(kx_columns), here, keepdims=False)
    planes = (count_y, 2 * kx_here, z_pad, y_rows)
    z_need = z_local + ORDER - 1 + (0 if z_local % 8 == 0 else 7)
    smem = pl.BlockSpec(memory_space=pltpu.SMEM)
    hbm = pl.BlockSpec(memory_space=pltpu.HBM)
    vmem = pl.BlockSpec(memory_space=pltpu.VMEM)

    def spread(state, batches, place, listed, origin):
        pieces = [(n, i) for n, array in enumerate(batches) for i in range(array.shape[0] // held)]
        opening = state is None
        return pl.pallas_call(
            lambda *refs: spread_kernel(
                *refs, pieces=pieces, origin=origin, listed=listed, points=points, z_local=z_local,
                y_local=y_local, count_y=count_y, kx_here=kx_here, z_need=z_need, y_rows=y_rows,
                chunk=math.gcd(atoms, 256), opening=opening,
            ),
            grid=(len(pieces),),
            in_specs=[smem, smem, pl.BlockSpec(kx_table.shape, lambda d: (0, 0))]
            + [hbm] * len(batches)
            + ([] if opening else [vmem, vmem]),
            out_specs=[vmem, vmem],
            out_shape=[pltpu.VMEM(planes, jnp.float32), pltpu.VMEM((devices, 8, qms), jnp.float32)],
            scratch_shapes=[
                pltpu.VMEM((ORDER, 2 * kx_here, atoms), jnp.float32),
                pltpu.VMEM((2, held, atoms), jnp.float32),
                pltpu.SemaphoreType.DMA((2,)),
            ],
            input_output_aliases={} if opening else {3 + len(batches): 0, 4 + len(batches): 1},
            compiler_params=pltpu.CompilerParams(
                dimension_semantics=("arbitrary",), vmem_limit_bytes=VMEM_BYTES
            ),
            cost_estimate=pl.CostEstimate(
                flops=len(pieces) * atoms * ORDER * parts_flops, bytes_accessed=0, transcendentals=0
            ),
            name="spread",
        )(here_row, place, kx_table, *batches, *([] if opening else state))

    parts_flops = 4 * z_rows * 2 * kx_here * y_rows
    if count_y == 2 and count_z % 4 == 0:
        spread_planes, qm_all = staged(record, count_z // 4, spread)
    else:
        records = lax.all_gather(record, AXES, axis=0, tiled=True)
        order = np.arange(devices)
        place = np.stack([order // count_y, order % count_y], axis=1).astype(np.int32)
        spread_planes, qm_all = spread(None, [records], jnp.asarray(place.reshape(-1)), 0, 0)
    constants = tables(points)
    third = points // RADIX

    def fixed(array):
        return pl.BlockSpec(array.shape, lambda k, n=array.ndim: (0,) * n)

    potential = pl.pallas_call(
        lambda *refs: transform_kernel(
            *refs, points=points, y_local=y_local, count_y=count_y, kx_here=kx_here, third=third
        ),
        grid=(kx_here,),
        in_specs=[smem, smem] + [fixed(array) for array in constants] + [vmem],
        out_specs=vmem,
        out_shape=pltpu.VMEM(planes, jnp.float32),
        input_output_aliases={2 + len(constants): 0},
        compiler_params=pltpu.CompilerParams(
            dimension_semantics=("arbitrary",), vmem_limit_bytes=VMEM_BYTES
        ),
        cost_estimate=pl.CostEstimate(flops=20_000_000_000, bytes_accessed=0, transcendentals=0),
        name="transform",
    )(here_row, jnp.asarray(kx_scalars.reshape(-1)), *constants, spread_planes)

    partial = pl.pallas_call(
        lambda *refs: force_kernel(
            *refs, points=points, z_local=z_local, count_y=count_y, kx_here=kx_here, z_rows=z_rows
        ),
        grid=(count_z,),
        in_specs=[pl.BlockSpec(kx_table.shape, lambda p: (0, 0)), vmem, vmem],
        out_specs=pl.BlockSpec((count_y, 3, qms), lambda p: (p, 0, 0)),
        out_shape=jax.ShapeDtypeStruct((devices, 3, qms), jnp.float32),
        compiler_params=pltpu.CompilerParams(
            dimension_semantics=("arbitrary",), vmem_limit_bytes=VMEM_BYTES
        ),
        name="forces",
    )(kx_table, qm_all, potential)
    moved = lax.all_to_all(partial, AXES, split_axis=0, concat_axis=0, tiled=True)
    return -qm_charge[None, :] * jnp.sum(moved, axis=0)


def solution(mesh):
    in_specs = (
        P(None, AXES),
        P(None, AXES),
        P(None, AXES),
        P(None, AXES),
        P(AXES),
    )
    out_specs = P(None, AXES)
    return jax.shard_map(shards, mesh=mesh, in_specs=in_specs, out_specs=out_specs, check_vma=False)
```

```python
import math

import jax
import jax.numpy as jnp
import numpy as np
from jax import lax
from jax.experimental import pallas as pl
from jax.experimental.pallas import tpu as pltpu
from jax.sharding import PartitionSpec as P

GRID = 384
ORDER = 4
SPLITTING = 0.8
AXES = ("gz", "gy")
RADIX = 3
VMEM_BYTES = 24 * 1024 * 1024


def round_up(value, unit):
    return -(-value // unit) * unit


def window_start(z_part, z_local):
    return pl.multiple_of(z_part * z_local // 8 * 8, 8)


def spline_weights(frac):
    remain = 1.0 - frac
    square = frac * frac
    cubed = square * frac
    values = [
        remain * remain * remain / 6.0,
        (3.0 * cubed - 6.0 * square + 4.0) / 6.0,
        (-3.0 * cubed + 3.0 * square + 3.0 * frac + 1.0) / 6.0,
        cubed / 6.0,
    ]
    slopes = [
        -0.5 * remain * remain,
        (3.0 * square - 4.0 * frac) / 2.0,
        (-3.0 * square + 2.0 * frac + 1.0) / 2.0,
        0.5 * square,
    ]
    return values, slopes


def sine_of_turns(turn):
    square = turn * turn
    total = jnp.full_like(turn, 0.0)
    for power in range(6, -1, -1):
        term = (-1.0) ** power * (2.0 * math.pi) ** (2 * power + 1) / math.factorial(2 * power + 1)
        total = total * square + term
    return total * turn


def cos_sin_of_turns(turn):
    folded = jnp.minimum(jnp.maximum(turn, -0.5 - turn), 0.5 - turn)
    return sine_of_turns(0.25 - jnp.abs(turn)), sine_of_turns(folded)


def halves(value):
    high = value.astype(jnp.bfloat16)
    low = (value - high.astype(jnp.float32)).astype(jnp.bfloat16)
    return high, low


def dot(left, right, contract=((1,), (0,))):
    return lax.dot_general(left, right, (contract, ((), ())), preferred_element_type=jnp.float32)


def x_phases(cells, kx_column, points):
    product = kx_column * cells
    turn = product * (1.0 / points)
    rest = product - points * jnp.floor(turn + 0.5)
    return cos_sin_of_turns(rest * (1.0 / points))


def record_kernel(weight_ref, base_ref, qm_base_ref, qm_frac_ref, out_ref):
    cells, atoms = weight_ref.shape
    out_ref[cells:, :] = jnp.zeros((out_ref.shape[0] - cells, atoms), jnp.float32)
    plane = lax.broadcasted_iota(jnp.int32, (ORDER, atoms), 0) - base_ref[0:1, :]
    choices = [(plane & (ORDER - 1)) == a for a in range(ORDER)]
    for n in range(ORDER * ORDER):
        four = jnp.zeros((ORDER, atoms), jnp.float32)
        for a in range(ORDER):
            row = a * ORDER * ORDER + n
            four = jnp.where(choices[a], weight_ref[row : row + 1, :], four)
        out_ref[n * ORDER : (n + 1) * ORDER, :] = four
    out_ref[cells : cells + 3, :] = base_ref[...].astype(jnp.float32)
    qms = qm_base_ref.shape[1]
    for n in range(6):
        line, lane = divmod(n * qms, atoms)
        line += cells + 3
        value = qm_base_ref[n : n + 1, :].astype(jnp.float32) if n < 3 else qm_frac_ref[n - 3 : n - 2, :]
        out_ref[line : line + 1, lane : lane + qms] = value


def spread_kernel(
    here_ref, place_ref, kx_ref, *refs, pieces, origin, listed, points, z_local, y_local, count_y, kx_here, z_need,
    y_rows, chunk, opening
):
    out_ref, qm_ref, phase_ref, slots, arrived = refs[-5:]
    step = pl.program_id(0)
    entry = 2 * (here_ref[0] * listed + origin + step)
    z_part = place_ref[entry]
    y_part = place_ref[entry + 1]
    held, atoms = slots.shape[1:]
    cells = ORDER**3
    parts = 2 * kx_here
    count = len(pieces)

    def fetch(n):
        array, block = pieces[n]
        source = refs[array].at[pl.ds(block * held, held)]
        return pltpu.make_async_copy(source, slots.at[n % 2], arrived.at[n % 2])

    @pl.when(step == 0)
    def _():
        fetch(0).start()
        if opening:
            out_ref[...] = jnp.zeros_like(out_ref)

    for n in range(1, count):

        @pl.when(step + 1 == n)
        def _():
            fetch(n).start()

    slot = step % 2
    pltpu.make_async_copy(refs[0].at[pl.ds(0, held)], slots.at[slot], arrived.at[slot]).wait()
    rec_ref = slots.at[slot]

    qms = qm_ref.shape[2]
    for n in range(6):
        line, lane = divmod(n * qms, atoms)
        line += cells + 3
        qm_ref[z_part * count_y + y_part, n : n + 1, :] = rec_ref[line : line + 1, lane : lane + qms]

    start = window_start(z_part, z_local)
    first_z = start.astype(jnp.float32)
    first_y = (y_part * y_local).astype(jnp.float32)
    short = kx_here % 2 == 0 and 0 < z_need % 8 <= 4
    assert y_rows <= 256
    groups = z_need // 8 if short else -(-z_need // 8)
    y_index = lax.broadcasted_iota(jnp.int32, (y_rows, chunk), 0).astype(jnp.float32).astype(jnp.bfloat16)
    one, none = jnp.ones((), jnp.bfloat16), jnp.zeros((), jnp.bfloat16)
    row = lax.broadcasted_iota(jnp.int32, (8, chunk), 0)

    def twice(value):
        return jnp.concatenate([value, value], axis=0).astype(jnp.bfloat16)[None]

    low_half = twice(jnp.where(row < 4, 1.0, 0.0))
    high_half = twice(jnp.where(row < 4, 0.0, 1.0))
    total = None
    for first in range(0, atoms, chunk):
        span = slice(first, first + chunk)
        base_cos, base_sin = x_phases(rec_ref[cells + 2 : cells + 3, span], kx_ref[:, 0:1], points)
        phase_ref[0, :kx_here, span] = base_cos
        phase_ref[0, kx_here:, span] = -base_sin
        for c in range(1, ORDER):
            turn_cos = kx_ref[:, 2 * c : 2 * c + 1]
            turn_sin = kx_ref[:, 2 * c + 1 : 2 * c + 2]
            phase_ref[c, :kx_here, span] = base_cos * turn_cos - base_sin * turn_sin
            phase_ref[c, kx_here:, span] = -(base_sin * turn_cos + base_cos * turn_sin)
        local_z = (rec_ref[cells : cells + 1, span] - first_z).astype(jnp.int32)
        local_y = rec_ref[cells + 1 : cells + 2, span] - first_y

        def mask(planes):
            return twice(jnp.where(((planes - local_z) & (-ORDER)) == 0, 1.0, 0.0))

        masks = [mask(row + 8 * m) for m in range(groups)]
        if short:
            last = mask((row & 3) + 8 * groups)
            lasts = (last * low_half, last * high_half)
        for b in range(ORDER):
            hits = jnp.where(y_index == (local_y + b).astype(jnp.bfloat16), one, none)
            weights = []
            for c in range(ORDER):
                place = (b * ORDER + c) * ORDER
                four = rec_ref[place : place + ORDER, span]
                weights.append(jnp.concatenate([four] * (8 // ORDER), axis=0))
            lines = []
            for n in range(parts):
                line = weights[0] * phase_ref[0, n : n + 1, span]
                for c in range(1, ORDER):
                    line = line + weights[c] * phase_ref[c, n : n + 1, span]
                lines.append(line)
            full = halves(jnp.concatenate(lines, axis=0))
            for i in range(2):
                tiles = full[i].reshape(kx_here, 16, chunk)
                stacked = [(tiles * m).reshape(16 * kx_here, chunk) for m in masks]
                if short:
                    pairs = tiles.reshape(kx_here // 2, 2, 16, chunk)
                    tiles = pairs[:, 0] * lasts[0] + pairs[:, 1] * lasts[1]
                    stacked.append(tiles.reshape(8 * kx_here, chunk))
                product = dot(jnp.concatenate(stacked, axis=0), hits, ((1,), (1,)))
                total = product if total is None else total + product
    for m in range(groups):
        for n in range(parts):
            row = (m * parts + n) * 8
            out_ref[y_part, n, pl.ds(start + 8 * m, 8), :] += total[row : row + 8]
    if short:
        for n in range(0, parts, 4):
            first = groups * parts * 8 + n * 4
            rows = pl.ds(start + 8 * groups, 8)
            zero = jnp.zeros((4, y_rows), jnp.float32)
            for i, m in enumerate((n, n + 2, n + 1, n + 3)):
                four = total[first + 4 * i : first + 4 * i + 4]
                out_ref[y_part, m, rows, :] += jnp.concatenate([four, zero], axis=0)


def split_dot(value, high, low):
    top, rest = halves(value)
    return dot(top, high) + (dot(rest, high) + dot(top, low))


def split_dot_left(high, low, value):
    top, rest = halves(value)
    return dot(high, top) + (dot(high, rest) + dot(low, top))


HALF_ROOT = math.sqrt(3.0) / 2.0


def three_way(parts, sign):
    (ar, ai), (br, bi), (cr, ci) = parts
    sum_r, sum_i = br + cr, bi + ci
    dif_r, dif_i = (br - cr) * HALF_ROOT, (bi - ci) * HALF_ROOT
    mid_r, mid_i = ar - 0.5 * sum_r, ai - 0.5 * sum_i
    return [
        (ar + sum_r, ai + sum_i),
        (mid_r - sign * dif_i, mid_i + sign * dif_r),
        (mid_r + sign * dif_i, mid_i - sign * dif_r),
    ]


def turned(value, cosine, sine, sign):
    re, im = value
    return (re * cosine - sign * (im * sine), im * cosine + sign * (re * sine))


def transform_kernel(
    here_ref, scal_ref, right_hi, right_lo, left_hi, left_lo, tw_row, tw_col, row_ref, col_ref,
    _, planes_ref, *, points, y_local, count_y, kx_here, third,
):
    index = pl.program_id(0)
    z_pad, y_rows = planes_ref.shape[2:]
    spare = z_pad - points

    def whole(part, n):
        line = None
        for q in range(count_y):
            body = planes_ref[q, part, n * third : (n + 1) * third, :]
            if n == 0:
                wrapped = planes_ref[q, part, points:, :]
                body = jnp.concatenate([body[:spare] + wrapped, body[spare:]], axis=0)
            if y_rows < points:
                body = jnp.concatenate(
                    [body, jnp.zeros((third, points - y_rows), jnp.float32)], axis=1
                )
            if q > 0:
                body = pltpu.roll(body, q * y_local, 1)
            line = body if line is None else line + body
        return line

    def lanes(value, part):
        return tuple(v[:, part * third : (part + 1) * third] for v in value)

    def row_turn(part, n, sign):
        if n == 0:
            return part
        return turned(part, tw_row[2 * n : 2 * n + 1, :], tw_row[2 * n + 1 : 2 * n + 2, :], sign)

    done = []
    for n in range(RADIX):
        rows = (whole(index, n), whole(index + kx_here, n))
        parts = three_way([lanes(rows, m) for m in range(RADIX)], -1.0)
        pieces = []
        for m, part in enumerate(parts):
            part = row_turn(part, m, -1.0)
            pieces.append(split_dot(jnp.concatenate(part, axis=1), right_hi[...], right_lo[...]))
        done.append(
            tuple(
                jnp.concatenate([p[:, i * third : (i + 1) * third] for p in pieces], axis=1)
                for i in range(2)
            )
        )
    parts = three_way(done, -1.0)
    entry = 2 * (here_ref[0] * kx_here + index)
    scale = scal_ref[entry]
    square = scal_ref[entry + 1]
    back = []
    for n, part in enumerate(parts):
        if n > 0:
            cosine = jnp.concatenate([tw_col[2 * n - 2]] * RADIX, axis=1)
            sine = jnp.concatenate([tw_col[2 * n - 1]] * RADIX, axis=1)
            part = turned(part, cosine, sine, -1.0)
        spectrum = split_dot_left(left_hi[...], left_lo[...], jnp.concatenate(part, axis=0))
        col_factor = jnp.concatenate([col_ref[0, n * third : (n + 1) * third, :]] * RADIX, axis=1)
        col_square = jnp.concatenate([col_ref[1, n * third : (n + 1) * third, :]] * RADIX, axis=1)
        total = col_square + row_ref[1:2, :] + square
        safe = jnp.where(total > 0.0, total, 1.0)
        green = jnp.where(total > 0.0, col_factor * row_ref[0:1, :] * scale / (math.pi * safe), 0.0)
        swapped = jnp.concatenate([spectrum[third:] * green, spectrum[:third] * green], axis=0)
        result = split_dot_left(left_hi[...], left_lo[...], swapped)
        part = (result[third:], result[:third])
        if n > 0:
            part = turned(part, cosine, sine, 1.0)
        back.append(part)
    back = three_way(back, 1.0)
    for n in range(RADIX):
        parts = []
        for m in range(RADIX):
            re, im = lanes(back[n], m)
            result = split_dot(jnp.concatenate([im, re], axis=1), right_hi[...], right_lo[...])
            parts.append(row_turn((result[:, third:], result[:, :third]), m, 1.0))
        parts = three_way(parts, 1.0)
        for i in range(2):
            value = jnp.concatenate([p[i] for p in parts], axis=1)
            for q in range(count_y):
                part = pltpu.roll(value, points - q * y_local, 1) if q > 0 else value
                part = part[:, :y_rows]
                held = index + i * kx_here
                planes_ref[q, held, n * third : (n + 1) * third, :] = part
                if n == 0:
                    planes_ref[q, held, points:, :] = part[:spare]


def force_kernel(
    kx_ref, qm_ref, pot_ref, out_ref, *, points, z_local, y_local, kx_here, z_rows, count_y
):
    z_part = pl.program_id(0)
    atoms = qm_ref.shape[2]
    start = window_start(z_part, z_local)
    first_z = start.astype(jnp.float32)
    y_rows = pot_ref.shape[3]
    y_need = round_up(y_local + ORDER - 1, 8)
    def placed(offset, weights):
        value = jnp.zeros(offset.shape, jnp.float32)
        for a in range(ORDER):
            value = jnp.where(offset == a, weights[a], value)
        return value

    for q in range(count_y):
        row = z_part * count_y + q
        local_z = (qm_ref[row, 0:1, :] - first_z).astype(jnp.int32)
        window = pot_ref[q, :, pl.ds(start, z_rows), :].reshape(2 * kx_here * z_rows, y_rows)
        top, rest = halves(window)
        local_y = qm_ref[row, 1:2, :].astype(jnp.int32) - q * y_local
        w_z, d_z = spline_weights(qm_ref[row, 3:4, :])
        w_y, d_y = spline_weights(qm_ref[row, 4:5, :])
        w_x, d_x = spline_weights(qm_ref[row, 5:6, :])
        offset_z = lax.broadcasted_iota(jnp.int32, (z_rows, atoms), 0) - local_z
        plane_w, plane_d = placed(offset_z, w_z)[None], placed(offset_z, d_z)[None]
        offset_y = lax.broadcasted_iota(jnp.int32, (y_need, atoms), 0) - local_y
        lines = jnp.concatenate([placed(offset_y, w_y), placed(offset_y, d_y)], axis=1)
        lines = jnp.concatenate([lines, jnp.zeros((y_rows - y_need, 2 * atoms), jnp.float32)], axis=0)
        row_hi, row_lo = halves(lines)
        along = dot(top, row_hi) + (dot(rest, row_hi) + dot(top, row_lo))
        along = along.reshape(2 * kx_here, z_rows, 2 * atoms)
        sum_z = jnp.sum(along[:, :, :atoms] * plane_d, axis=1)
        sum_y = jnp.sum(along[:, :, atoms:] * plane_w, axis=1)
        sum_x = jnp.sum(along[:, :, :atoms] * plane_w, axis=1)
        base_cos, base_sin = x_phases(qm_ref[row, 2:3, :], kx_ref[:, 0:1], points)
        line_w = [w_x[0] * base_cos, w_x[0] * base_sin]
        line_d = [d_x[0] * base_cos, d_x[0] * base_sin]
        for c in range(1, ORDER):
            turn_cos = kx_ref[:, 2 * c : 2 * c + 1]
            turn_sin = kx_ref[:, 2 * c + 1 : 2 * c + 2]
            cosine = base_cos * turn_cos - base_sin * turn_sin
            sine = base_sin * turn_cos + base_cos * turn_sin
            line_w = [line_w[0] + w_x[c] * cosine, line_w[1] + w_x[c] * sine]
            line_d = [line_d[0] + d_x[c] * cosine, line_d[1] + d_x[c] * sine]
        line_w = jnp.concatenate([line_w[0], -line_w[1]], axis=0)
        line_d = jnp.concatenate([line_d[0], -line_d[1]], axis=0)
        out_ref[q, 0:1, :] = jnp.sum(sum_z * line_w, axis=0, keepdims=True)
        out_ref[q, 1:2, :] = jnp.sum(sum_y * line_w, axis=0, keepdims=True)
        out_ref[q, 2:3, :] = jnp.sum(sum_x * line_d, axis=0, keepdims=True)


def tables(points):
    third = points // RADIX
    index = np.arange(third)
    angle = 2.0 * np.pi / third * (np.outer(index, index) % third)
    cosine, sine = np.cos(angle), np.sin(angle)
    right = np.block([[cosine, -sine], [sine, cosine]])
    left = np.block([[cosine, sine], [-sine, cosine]])

    def split(matrix):
        value = jnp.asarray(matrix, jnp.float32)
        high = jnp.asarray(matrix.astype(jnp.bfloat16))
        low = jnp.asarray((matrix - matrix.astype(jnp.bfloat16).astype(np.float64)).astype(jnp.bfloat16))
        return high, low

    turn = 2.0 * np.pi / points * np.outer(np.arange(RADIX), index)
    twiddle = np.stack([np.cos(turn), np.sin(turn)], axis=1).reshape(2 * RADIX, third).astype(np.float32)
    tw_row = jnp.asarray(twiddle)
    tw_col = jnp.asarray(np.broadcast_to(twiddle[2:, :, None], (2 * RADIX - 2, third, third)).copy())
    slots = (RADIX * np.arange(third)[None, :] + np.arange(RADIX)[:, None]).reshape(-1)
    factor, square = factors(slots, points)
    row = jnp.asarray(np.stack([factor, square]).astype(np.float32))
    col = jnp.asarray(
        np.broadcast_to(np.stack([factor, square])[:, :, None], (2, points, third)).astype(np.float32)
    )
    return split(right) + split(left) + (tw_row, tw_col, row, col)


def kx_tables(devices, kx_here, points):
    kx = np.arange(devices * kx_here)
    turn = 2.0 * np.pi / points * (kx[:, None] * np.arange(ORDER)[None, :] % points)
    columns = np.stack([np.cos(turn), np.sin(turn)], axis=2).reshape(-1, 2 * ORDER)
    columns[:, 0] = kx
    factor, square = factors(kx, points)
    factor = np.where(kx < points // 2, factor, 0.0) * np.where(kx == 0, 1.0, 2.0) / float(points) ** 3
    scalars = np.stack([factor, square], axis=1)
    shape = (devices, kx_here, -1)
    return columns.reshape(shape).astype(np.float32), scalars.reshape(shape).astype(np.float32)


def factors(index, points):
    signed = np.where(index < points // 2, index, index - points) / points
    spline = 2.0 / 3.0 + np.cos(2.0 * np.pi * index / points) / 3.0
    factor = np.exp(-((np.pi / SPLITTING) ** 2) * signed**2) / spline**2
    return np.where(index == points // 2, 0.0, factor), signed**2


def staged(record, outer, spread):
    def index(where):
        z, x, core, y = where
        return ((z * 2 + x) * 2 + core) * 2 + y

    everyone = [(z, x, c, y) for z in range(outer) for x in range(2) for c in range(2) for y in range(2)]

    def across(w, over_x):
        return (w[0], 1 - w[1], w[2], w[3]) if over_x else (w[0], w[1], w[2], 1 - w[3])

    def flip_one(w):
        return across(w, w[2] == 0)

    def flip_two(w):
        return across(w, w[2] == 1)

    def partner(w):
        return (w[0], w[1], 1 - w[2], w[3])

    def moved(batch, sender):
        array, sources = batch
        route = [(index(sender(w)), index(w)) for w in everyone]
        return lax.ppermute(array, AXES, route), [lambda w, s=s: s(sender(w)) for s in sources]

    def after(state, batches):
        arrays, state = lax.optimization_barrier(([b[0] for b in batches], state))
        return state, [(array, b[1]) for array, b in zip(arrays, batches)]

    def together(batches):
        return jnp.concatenate([b[0] for b in batches], axis=0), [s for b in batches for s in b[1]]

    mine = (record, [lambda w: w])
    shift = [
        moved(mine, lambda w, n=n: ((w[0] - n) % outer, w[1], w[2], w[3])) for n in range(1, outer)
    ]
    other = moved(mine, partner)
    one, two = moved(mine, flip_one), moved(mine, flip_two)

    def names(sources, sender=lambda w: w):
        return [lambda w, s=s: s(sender(w)) for s in sources]

    def chain(*senders):
        def source(w):
            for sender in senders:
                w = sender(w)
            return w

        return source

    shifts = [s for batch in shift for s in batch[1]]
    listed = (
        [lambda w: w, partner, flip_one, flip_two, chain(partner, flip_one), chain(partner, flip_two)]
        + [chain(flip_two, flip_one)] + shifts
        + [chain(partner, flip_two, flip_one)] + names(shifts, partner)
        + names(shifts, flip_one) + names(shifts, flip_two)
        + names(shifts, chain(partner, flip_one)) + names(shifts, chain(partner, flip_two))
        + names(shifts, chain(flip_two, flip_one)) + names(shifts, chain(partner, flip_two, flip_one))
    )
    parts = [[(index(s(w)) // 2, index(s(w)) % 2) for s in listed] for w in everyone]
    assert all(len(set(row)) == len(everyone) for row in parts)
    place = jnp.asarray(np.asarray(parts, np.int32).reshape(-1))
    origin = 0

    def add(state, batches):
        nonlocal origin
        first = origin
        for _, sources in batches:
            for source in sources:
                assert all(source(w) == listed[origin](w) for w in everyone)
                origin += 1
        return spread(state, [batch[0] for batch in batches], place, len(listed), first)

    state = add(None, [mine, other])
    state, (one, two) = after(state, [one, two])
    both = moved(one, flip_two)
    one_partner, two_partner = moved(one, partner), moved(two, partner)
    state = add(state, [one, two])
    state = add(state, [one_partner, two_partner])
    state, (both, *shift) = after(state, [both] + shift)
    shift = together(shift)
    shift_one, shift_two = moved(shift, flip_one), moved(shift, flip_two)
    both_partner, shift_partner = moved(both, partner), moved(shift, partner)
    state = add(state, [both, shift])
    state = add(state, [both_partner, shift_partner])
    state, (shift_one, shift_two) = after(state, [shift_one, shift_two])
    shift_both = moved(shift_one, flip_two)
    one_partner, two_partner = moved(shift_one, partner), moved(shift_two, partner)
    state = add(state, [shift_one, shift_two])
    state, (shift_both,) = after(state, [shift_both])
    both_partner = moved(shift_both, partner)
    state = add(state, [one_partner, two_partner])
    return add(state, [shift_both, both_partner])


def shards(spread_weights, spread_base, qm_base, qm_frac, qm_charge):
    points = GRID
    count_z = lax.axis_size("gz")
    count_y = lax.axis_size("gy")
    devices = count_z * count_y
    z_local = points // count_z
    y_local = points // count_y
    kx_here = -(-(points // 2) // devices)
    here = lax.axis_index("gz") * count_y + lax.axis_index("gy")
    z_rows = round_up(z_local + ORDER - 1 + (0 if z_local % 8 == 0 else 7), 8)
    z_pad = (points - z_local) // 8 * 8 + z_rows
    y_rows = min(round_up(y_local + ORDER - 1, 128), points)

    atoms = spread_weights.shape[1]
    qms = qm_charge.shape[0]
    lines = -(-6 * qms // atoms)
    held = round_up(ORDER**3 + 3 + lines, 8)
    record = pl.pallas_call(
        record_kernel,
        out_shape=jax.ShapeDtypeStruct((held, atoms), jnp.float32),
        name="record",
    )(spread_weights, spread_base, qm_base, qm_frac)

    kx_columns, kx_scalars = kx_tables(devices, kx_here, points)
    here_row = here.astype(jnp.int32).reshape(1)
    kx_table = lax.dynamic_index_in_dim(jnp.asarray(kx_columns), here, keepdims=False)
    planes = (count_y, 2 * kx_here, z_pad, y_rows)
    z_need = z_local + ORDER - 1 + (0 if z_local % 8 == 0 else 7)
    smem = pl.BlockSpec(memory_space=pltpu.SMEM)
    hbm = pl.BlockSpec(memory_space=pltpu.HBM)
    vmem = pl.BlockSpec(memory_space=pltpu.VMEM)

    def spread(state, batches, place, listed, origin):
        pieces = [(n, i) for n, array in enumerate(batches) for i in range(array.shape[0] // held)]
        opening = state is None
        return pl.pallas_call(
            lambda *refs: spread_kernel(
                *refs, pieces=pieces, origin=origin, listed=listed, points=points, z_local=z_local,
                y_local=y_local, count_y=count_y, kx_here=kx_here, z_need=z_need, y_rows=y_rows,
                chunk=math.gcd(atoms, 256), opening=opening,
            ),
            grid=(len(pieces),),
            in_specs=[smem, smem, pl.BlockSpec(kx_table.shape, lambda d: (0, 0))]
            + [hbm] * len(batches)
            + ([] if opening else [vmem, vmem]),
            out_specs=[vmem, vmem],
            out_shape=[pltpu.VMEM(planes, jnp.float32), pltpu.VMEM((devices, 8, qms), jnp.float32)],
            scratch_shapes=[
                pltpu.VMEM((ORDER, 2 * kx_here, atoms), jnp.float32),
                pltpu.VMEM((2, held, atoms), jnp.float32),
                pltpu.SemaphoreType.DMA((2,)),
            ],
            input_output_aliases={} if opening else {3 + len(batches): 0, 4 + len(batches): 1},
            compiler_params=pltpu.CompilerParams(
                dimension_semantics=("arbitrary",), vmem_limit_bytes=VMEM_BYTES
            ),
            cost_estimate=pl.CostEstimate(
                flops=len(pieces) * atoms * ORDER * parts_flops, bytes_accessed=0, transcendentals=0
            ),
            name="spread",
        )(here_row, place, kx_table, *batches, *([] if opening else state))

    parts_flops = 4 * z_rows * 2 * kx_here * y_rows
    if count_y == 2 and count_z % 4 == 0:
        spread_planes, qm_all = staged(record, count_z // 4, spread)
    else:
        records = lax.all_gather(record, AXES, axis=0, tiled=True)
        order = np.arange(devices)
        place = np.stack([order // count_y, order % count_y], axis=1).astype(np.int32)
        spread_planes, qm_all = spread(None, [records], jnp.asarray(place.reshape(-1)), 0, 0)
    constants = tables(points)
    third = points // RADIX

    def fixed(array):
        return pl.BlockSpec(array.shape, lambda k, n=array.ndim: (0,) * n)

    potential = pl.pallas_call(
        lambda *refs: transform_kernel(
            *refs, points=points, y_local=y_local, count_y=count_y, kx_here=kx_here, third=third
        ),
        grid=(kx_here,),
        in_specs=[smem, smem] + [fixed(array) for array in constants] + [vmem],
        out_specs=vmem,
        out_shape=pltpu.VMEM(planes, jnp.float32),
        input_output_aliases={2 + len(constants): 0},
        compiler_params=pltpu.CompilerParams(
            dimension_semantics=("arbitrary",), vmem_limit_bytes=VMEM_BYTES
        ),
        cost_estimate=pl.CostEstimate(flops=20_000_000_000, bytes_accessed=0, transcendentals=0),
        name="transform",
    )(here_row, jnp.asarray(kx_scalars.reshape(-1)), *constants, spread_planes)

    partial = pl.pallas_call(
        lambda *refs: force_kernel(
            *refs, points=points, z_local=z_local, y_local=y_local, count_y=count_y,
            kx_here=kx_here, z_rows=z_rows,
        ),
        grid=(count_z,),
        in_specs=[pl.BlockSpec(kx_table.shape, lambda p: (0, 0)), vmem, vmem],
        out_specs=pl.BlockSpec((count_y, 3, qms), lambda p: (p, 0, 0)),
        out_shape=jax.ShapeDtypeStruct((devices, 3, qms), jnp.float32),
        compiler_params=pltpu.CompilerParams(
            dimension_semantics=("arbitrary",), vmem_limit_bytes=VMEM_BYTES
        ),
        name="forces",
    )(kx_table, qm_all, potential)
    moved = lax.all_to_all(partial, AXES, split_axis=0, concat_axis=0, tiled=True)
    return -qm_charge[None, :] * jnp.sum(moved, axis=0)


def solution(mesh):
    in_specs = (
        P(None, AXES),
        P(None, AXES),
        P(None, AXES),
        P(None, AXES),
        P(AXES),
    )
    out_specs = P(None, AXES)
    return jax.shard_map(shards, mesh=mesh, in_specs=in_specs, out_specs=out_specs, check_vma=False)
```

```python
import math

import jax
import jax.numpy as jnp
import numpy as np
from jax import lax
from jax.experimental import pallas as pl
from jax.experimental.pallas import tpu as pltpu
from jax.sharding import PartitionSpec as P

GRID = 384
ORDER = 4
SPLITTING = 0.8
AXES = ("gz", "gy")
RADIX = 3
VMEM_BYTES = 24 * 1024 * 1024


def round_up(value, unit):
    return -(-value // unit) * unit


def window_start(z_part, z_local):
    return pl.multiple_of(z_part * z_local // 8 * 8, 8)


def spline_weights(frac):
    remain = 1.0 - frac
    square = frac * frac
    cubed = square * frac
    values = [
        remain * remain * remain / 6.0,
        (3.0 * cubed - 6.0 * square + 4.0) / 6.0,
        (-3.0 * cubed + 3.0 * square + 3.0 * frac + 1.0) / 6.0,
        cubed / 6.0,
    ]
    slopes = [
        -0.5 * remain * remain,
        (3.0 * square - 4.0 * frac) / 2.0,
        (-3.0 * square + 2.0 * frac + 1.0) / 2.0,
        0.5 * square,
    ]
    return values, slopes


def sine_of_turns(turn):
    square = turn * turn
    total = jnp.full_like(turn, 0.0)
    for power in range(6, -1, -1):
        term = (-1.0) ** power * (2.0 * math.pi) ** (2 * power + 1) / math.factorial(2 * power + 1)
        total = total * square + term
    return total * turn


def cos_sin_of_turns(turn):
    folded = jnp.minimum(jnp.maximum(turn, -0.5 - turn), 0.5 - turn)
    return sine_of_turns(0.25 - jnp.abs(turn)), sine_of_turns(folded)


def halves(value):
    high = value.astype(jnp.bfloat16)
    low = (value - high.astype(jnp.float32)).astype(jnp.bfloat16)
    return high, low


def dot(left, right, contract=((1,), (0,))):
    return lax.dot_general(left, right, (contract, ((), ())), preferred_element_type=jnp.float32)


def x_phases(cells, kx_column, points):
    product = kx_column * cells
    turn = product * (1.0 / points)
    rest = product - points * jnp.floor(turn + 0.5)
    return cos_sin_of_turns(rest * (1.0 / points))


def record_kernel(weight_ref, base_ref, qm_base_ref, qm_frac_ref, out_ref):
    cells, atoms = weight_ref.shape
    out_ref[cells:, :] = jnp.zeros((out_ref.shape[0] - cells, atoms), jnp.float32)
    plane = lax.broadcasted_iota(jnp.int32, (ORDER, atoms), 0) - base_ref[0:1, :]
    choices = [(plane & (ORDER - 1)) == a for a in range(ORDER)]
    for n in range(ORDER * ORDER):
        four = jnp.zeros((ORDER, atoms), jnp.float32)
        for a in range(ORDER):
            row = a * ORDER * ORDER + n
            four = jnp.where(choices[a], weight_ref[row : row + 1, :], four)
        out_ref[n * ORDER : (n + 1) * ORDER, :] = four
    out_ref[cells : cells + 3, :] = base_ref[...].astype(jnp.float32)
    qms = qm_base_ref.shape[1]
    for n in range(6):
        line, lane = divmod(n * qms, atoms)
        line += cells + 3
        value = qm_base_ref[n : n + 1, :].astype(jnp.float32) if n < 3 else qm_frac_ref[n - 3 : n - 2, :]
        out_ref[line : line + 1, lane : lane + qms] = value


def spread_kernel(
    here_ref, place_ref, kx_all, *refs, pieces, origin, listed, points, z_local, y_local, count_y, kx_here, z_need,
    y_rows, chunk, opening
):
    out_ref, qm_ref, phase_ref, slots, arrived = refs[-5:]
    step = pl.program_id(0)
    entry = 2 * (here_ref[0] * listed + origin + step)
    z_part = place_ref[entry]
    y_part = place_ref[entry + 1]
    held, atoms = slots.shape[1:]
    cells = ORDER**3
    parts = 2 * kx_here
    count = len(pieces)
    kx_ref = kx_all.at[here_ref[0]]

    def fetch(n):
        array, block = pieces[n]
        source = refs[array].at[pl.ds(block * held, held)]
        return pltpu.make_async_copy(source, slots.at[n % 2], arrived.at[n % 2])

    @pl.when(step == 0)
    def _():
        fetch(0).start()
        if opening:
            out_ref[...] = jnp.zeros_like(out_ref)

    for n in range(1, count):

        @pl.when(step + 1 == n)
        def _():
            fetch(n).start()

    slot = step % 2
    pltpu.make_async_copy(refs[0].at[pl.ds(0, held)], slots.at[slot], arrived.at[slot]).wait()
    rec_ref = slots.at[slot]

    qms = qm_ref.shape[2]
    for n in range(6):
        line, lane = divmod(n * qms, atoms)
        line += cells + 3
        qm_ref[z_part * count_y + y_part, n : n + 1, :] = rec_ref[line : line + 1, lane : lane + qms]

    start = window_start(z_part, z_local)
    first_z = start.astype(jnp.float32)
    first_y = (y_part * y_local).astype(jnp.float32)
    short = kx_here % 2 == 0 and 0 < z_need % 8 <= 4
    assert y_rows <= 256
    groups = z_need // 8 if short else -(-z_need // 8)
    y_index = lax.broadcasted_iota(jnp.int32, (y_rows, chunk), 0).astype(jnp.float32).astype(jnp.bfloat16)
    one, none = jnp.ones((), jnp.bfloat16), jnp.zeros((), jnp.bfloat16)
    row = lax.broadcasted_iota(jnp.int32, (8, chunk), 0)

    def twice(value):
        return jnp.concatenate([value, value], axis=0).astype(jnp.bfloat16)[None]

    low_half = twice(jnp.where(row < 4, 1.0, 0.0))
    high_half = twice(jnp.where(row < 4, 0.0, 1.0))
    total = None
    for first in range(0, atoms, chunk):
        span = slice(first, first + chunk)
        base_cos, base_sin = x_phases(rec_ref[cells + 2 : cells + 3, span], kx_ref[:, 0:1], points)
        phase_ref[0, :kx_here, span] = base_cos
        phase_ref[0, kx_here:, span] = -base_sin
        for c in range(1, ORDER):
            turn_cos = kx_ref[:, 2 * c : 2 * c + 1]
            turn_sin = kx_ref[:, 2 * c + 1 : 2 * c + 2]
            phase_ref[c, :kx_here, span] = base_cos * turn_cos - base_sin * turn_sin
            phase_ref[c, kx_here:, span] = -(base_sin * turn_cos + base_cos * turn_sin)
        local_z = (rec_ref[cells : cells + 1, span] - first_z).astype(jnp.int32)
        local_y = rec_ref[cells + 1 : cells + 2, span] - first_y

        def mask(planes):
            return twice(jnp.where(((planes - local_z) & (-ORDER)) == 0, 1.0, 0.0))

        masks = [mask(row + 8 * m) for m in range(groups)]
        if short:
            last = mask((row & 3) + 8 * groups)
            lasts = (last * low_half, last * high_half)
        for b in range(ORDER):
            hits = jnp.where(y_index == (local_y + b).astype(jnp.bfloat16), one, none)
            weights = []
            for c in range(ORDER):
                place = (b * ORDER + c) * ORDER
                four = rec_ref[place : place + ORDER, span]
                weights.append(jnp.concatenate([four] * (8 // ORDER), axis=0))
            lines = []
            for n in range(parts):
                line = weights[0] * phase_ref[0, n : n + 1, span]
                for c in range(1, ORDER):
                    line = line + weights[c] * phase_ref[c, n : n + 1, span]
                lines.append(line)
            full = halves(jnp.concatenate(lines, axis=0))
            for i in range(2):
                tiles = full[i].reshape(kx_here, 16, chunk)
                stacked = [(tiles * m).reshape(16 * kx_here, chunk) for m in masks]
                if short:
                    pairs = tiles.reshape(kx_here // 2, 2, 16, chunk)
                    tiles = pairs[:, 0] * lasts[0] + pairs[:, 1] * lasts[1]
                    stacked.append(tiles.reshape(8 * kx_here, chunk))
                product = dot(jnp.concatenate(stacked, axis=0), hits, ((1,), (1,)))
                total = product if total is None else total + product
    for m in range(groups):
        for n in range(parts):
            row = (m * parts + n) * 8
            out_ref[y_part, n, pl.ds(start + 8 * m, 8), :] += total[row : row + 8]
    if short:
        for n in range(0, parts, 4):
            first = groups * parts * 8 + n * 4
            rows = pl.ds(start + 8 * groups, 8)
            zero = jnp.zeros((4, y_rows), jnp.float32)
            for i, m in enumerate((n, n + 2, n + 1, n + 3)):
                four = total[first + 4 * i : first + 4 * i + 4]
                out_ref[y_part, m, rows, :] += jnp.concatenate([four, zero], axis=0)


def split_dot(value, high, low):
    top, rest = halves(value)
    return dot(top, high) + (dot(rest, high) + dot(top, low))


def split_dot_left(high, low, value):
    top, rest = halves(value)
    return dot(high, top) + (dot(high, rest) + dot(low, top))


HALF_ROOT = math.sqrt(3.0) / 2.0


def three_way(parts, sign):
    (ar, ai), (br, bi), (cr, ci) = parts
    sum_r, sum_i = br + cr, bi + ci
    dif_r, dif_i = (br - cr) * HALF_ROOT, (bi - ci) * HALF_ROOT
    mid_r, mid_i = ar - 0.5 * sum_r, ai - 0.5 * sum_i
    return [
        (ar + sum_r, ai + sum_i),
        (mid_r - sign * dif_i, mid_i + sign * dif_r),
        (mid_r + sign * dif_i, mid_i - sign * dif_r),
    ]


def turned(value, cosine, sine, sign):
    re, im = value
    return (re * cosine - sign * (im * sine), im * cosine + sign * (re * sine))


def transform_kernel(
    here_ref, scal_ref, right_hi, right_lo, left_hi, left_lo, tw_row, tw_col, row_ref, col_ref,
    _, planes_ref, *, points, y_local, count_y, kx_here, third,
):
    index = pl.program_id(0)
    z_pad, y_rows = planes_ref.shape[2:]
    spare = z_pad - points

    def whole(part, n):
        line = None
        for q in range(count_y):
            body = planes_ref[q, part, n * third : (n + 1) * third, :]
            if n == 0:
                wrapped = planes_ref[q, part, points:, :]
                body = jnp.concatenate([body[:spare] + wrapped, body[spare:]], axis=0)
            if y_rows < points:
                body = jnp.concatenate(
                    [body, jnp.zeros((third, points - y_rows), jnp.float32)], axis=1
                )
            if q > 0:
                body = pltpu.roll(body, q * y_local, 1)
            line = body if line is None else line + body
        return line

    def lanes(value, part):
        return tuple(v[:, part * third : (part + 1) * third] for v in value)

    def row_turn(part, n, sign):
        if n == 0:
            return part
        return turned(part, tw_row[2 * n : 2 * n + 1, :], tw_row[2 * n + 1 : 2 * n + 2, :], sign)

    done = []
    for n in range(RADIX):
        rows = (whole(index, n), whole(index + kx_here, n))
        parts = three_way([lanes(rows, m) for m in range(RADIX)], -1.0)
        pieces = []
        for m, part in enumerate(parts):
            part = row_turn(part, m, -1.0)
            pieces.append(split_dot(jnp.concatenate(part, axis=1), right_hi[...], right_lo[...]))
        done.append(
            tuple(
                jnp.concatenate([p[:, i * third : (i + 1) * third] for p in pieces], axis=1)
                for i in range(2)
            )
        )
    parts = three_way(done, -1.0)
    entry = 2 * (here_ref[0] * kx_here + index)
    scale = scal_ref[entry]
    square = scal_ref[entry + 1]
    back = []
    for n, part in enumerate(parts):
        if n > 0:
            cosine = jnp.concatenate([tw_col[2 * n - 2]] * RADIX, axis=1)
            sine = jnp.concatenate([tw_col[2 * n - 1]] * RADIX, axis=1)
            part = turned(part, cosine, sine, -1.0)
        spectrum = split_dot_left(left_hi[...], left_lo[...], jnp.concatenate(part, axis=0))
        col_factor = jnp.concatenate([col_ref[0, n * third : (n + 1) * third, :]] * RADIX, axis=1)
        col_square = jnp.concatenate([col_ref[1, n * third : (n + 1) * third, :]] * RADIX, axis=1)
        total = col_square + row_ref[1:2, :] + square
        safe = jnp.where(total > 0.0, total, 1.0)
        green = jnp.where(total > 0.0, col_factor * row_ref[0:1, :] * scale / (math.pi * safe), 0.0)
        swapped = jnp.concatenate([spectrum[third:] * green, spectrum[:third] * green], axis=0)
        result = split_dot_left(left_hi[...], left_lo[...], swapped)
        part = (result[third:], result[:third])
        if n > 0:
            part = turned(part, cosine, sine, 1.0)
        back.append(part)
    back = three_way(back, 1.0)
    for n in range(RADIX):
        parts = []
        for m in range(RADIX):
            re, im = lanes(back[n], m)
            result = split_dot(jnp.concatenate([im, re], axis=1), right_hi[...], right_lo[...])
            parts.append(row_turn((result[:, third:], result[:, :third]), m, 1.0))
        parts = three_way(parts, 1.0)
        for i in range(2):
            value = jnp.concatenate([p[i] for p in parts], axis=1)
            for q in range(count_y):
                part = pltpu.roll(value, points - q * y_local, 1) if q > 0 else value
                part = part[:, :y_rows]
                held = index + i * kx_here
                planes_ref[q, held, n * third : (n + 1) * third, :] = part
                if n == 0:
                    planes_ref[q, held, points:, :] = part[:spare]


def force_kernel(
    here_ref, kx_all, qm_ref, pot_ref, out_ref, *, points, z_local, y_local, kx_here, z_rows, count_y
):
    z_part = pl.program_id(0)
    kx_ref = kx_all.at[here_ref[0]]
    atoms = qm_ref.shape[2]
    start = window_start(z_part, z_local)
    first_z = start.astype(jnp.float32)
    y_rows = pot_ref.shape[3]
    y_need = round_up(y_local + ORDER - 1, 8)
    def placed(offset, weights):
        value = jnp.zeros(offset.shape, jnp.float32)
        for a in range(ORDER):
            value = jnp.where(offset == a, weights[a], value)
        return value

    for q in range(count_y):
        row = z_part * count_y + q
        local_z = (qm_ref[row, 0:1, :] - first_z).astype(jnp.int32)
        window = pot_ref[q, :, pl.ds(start, z_rows), :].reshape(2 * kx_here * z_rows, y_rows)
        top, rest = halves(window)
        local_y = qm_ref[row, 1:2, :].astype(jnp.int32) - q * y_local
        w_z, d_z = spline_weights(qm_ref[row, 3:4, :])
        w_y, d_y = spline_weights(qm_ref[row, 4:5, :])
        w_x, d_x = spline_weights(qm_ref[row, 5:6, :])
        offset_z = lax.broadcasted_iota(jnp.int32, (z_rows, atoms), 0) - local_z
        plane_w, plane_d = placed(offset_z, w_z)[None], placed(offset_z, d_z)[None]
        offset_y = lax.broadcasted_iota(jnp.int32, (y_need, atoms), 0) - local_y
        lines = jnp.concatenate([placed(offset_y, w_y), placed(offset_y, d_y)], axis=1)
        lines = jnp.concatenate([lines, jnp.zeros((y_rows - y_need, 2 * atoms), jnp.float32)], axis=0)
        row_hi, row_lo = halves(lines)
        along = dot(top, row_hi) + (dot(rest, row_hi) + dot(top, row_lo))
        along = along.reshape(2 * kx_here, z_rows, 2 * atoms)
        sum_z = jnp.sum(along[:, :, :atoms] * plane_d, axis=1)
        sum_y = jnp.sum(along[:, :, atoms:] * plane_w, axis=1)
        sum_x = jnp.sum(along[:, :, :atoms] * plane_w, axis=1)
        base_cos, base_sin = x_phases(qm_ref[row, 2:3, :], kx_ref[:, 0:1], points)
        line_w = [w_x[0] * base_cos, w_x[0] * base_sin]
        line_d = [d_x[0] * base_cos, d_x[0] * base_sin]
        for c in range(1, ORDER):
            turn_cos = kx_ref[:, 2 * c : 2 * c + 1]
            turn_sin = kx_ref[:, 2 * c + 1 : 2 * c + 2]
            cosine = base_cos * turn_cos - base_sin * turn_sin
            sine = base_sin * turn_cos + base_cos * turn_sin
            line_w = [line_w[0] + w_x[c] * cosine, line_w[1] + w_x[c] * sine]
            line_d = [line_d[0] + d_x[c] * cosine, line_d[1] + d_x[c] * sine]
        line_w = jnp.concatenate([line_w[0], -line_w[1]], axis=0)
        line_d = jnp.concatenate([line_d[0], -line_d[1]], axis=0)
        out_ref[q, 0:1, :] = jnp.sum(sum_z * line_w, axis=0, keepdims=True)
        out_ref[q, 1:2, :] = jnp.sum(sum_y * line_w, axis=0, keepdims=True)
        out_ref[q, 2:3, :] = jnp.sum(sum_x * line_d, axis=0, keepdims=True)


def tables(points):
    third = points // RADIX
    index = np.arange(third)
    angle = 2.0 * np.pi / third * (np.outer(index, index) % third)
    cosine, sine = np.cos(angle), np.sin(angle)
    right = np.block([[cosine, -sine], [sine, cosine]])
    left = np.block([[cosine, sine], [-sine, cosine]])

    def split(matrix):
        value = jnp.asarray(matrix, jnp.float32)
        high = jnp.asarray(matrix.astype(jnp.bfloat16))
        low = jnp.asarray((matrix - matrix.astype(jnp.bfloat16).astype(np.float64)).astype(jnp.bfloat16))
        return high, low

    turn = 2.0 * np.pi / points * np.outer(np.arange(RADIX), index)
    twiddle = np.stack([np.cos(turn), np.sin(turn)], axis=1).reshape(2 * RADIX, third).astype(np.float32)
    tw_row = jnp.asarray(twiddle)
    tw_col = jnp.asarray(np.broadcast_to(twiddle[2:, :, None], (2 * RADIX - 2, third, third)).copy())
    slots = (RADIX * np.arange(third)[None, :] + np.arange(RADIX)[:, None]).reshape(-1)
    factor, square = factors(slots, points)
    row = jnp.asarray(np.stack([factor, square]).astype(np.float32))
    col = jnp.asarray(
        np.broadcast_to(np.stack([factor, square])[:, :, None], (2, points, third)).astype(np.float32)
    )
    return split(right) + split(left) + (tw_row, tw_col, row, col)


def kx_tables(devices, kx_here, points):
    kx = np.arange(devices * kx_here)
    turn = 2.0 * np.pi / points * (kx[:, None] * np.arange(ORDER)[None, :] % points)
    columns = np.stack([np.cos(turn), np.sin(turn)], axis=2).reshape(-1, 2 * ORDER)
    columns[:, 0] = kx
    factor, square = factors(kx, points)
    factor = np.where(kx < points // 2, factor, 0.0) * np.where(kx == 0, 1.0, 2.0) / float(points) ** 3
    scalars = np.stack([factor, square], axis=1)
    shape = (devices, kx_here, -1)
    return columns.reshape(shape).astype(np.float32), scalars.reshape(shape).astype(np.float32)


def factors(index, points):
    signed = np.where(index < points // 2, index, index - points) / points
    spline = 2.0 / 3.0 + np.cos(2.0 * np.pi * index / points) / 3.0
    factor = np.exp(-((np.pi / SPLITTING) ** 2) * signed**2) / spline**2
    return np.where(index == points // 2, 0.0, factor), signed**2


def staged(record, outer, spread):
    def index(where):
        z, x, core, y = where
        return ((z * 2 + x) * 2 + core) * 2 + y

    everyone = [(z, x, c, y) for z in range(outer) for x in range(2) for c in range(2) for y in range(2)]

    def across(w, over_x):
        return (w[0], 1 - w[1], w[2], w[3]) if over_x else (w[0], w[1], w[2], 1 - w[3])

    def flip_one(w):
        return across(w, w[2] == 0)

    def flip_two(w):
        return across(w, w[2] == 1)

    def partner(w):
        return (w[0], w[1], 1 - w[2], w[3])

    def moved(batch, sender):
        array, sources = batch
        route = [(index(sender(w)), index(w)) for w in everyone]
        return lax.ppermute(array, AXES, route), [lambda w, s=s: s(sender(w)) for s in sources]

    def after(state, batches):
        arrays, state = lax.optimization_barrier(([b[0] for b in batches], state))
        return state, [(array, b[1]) for array, b in zip(arrays, batches)]

    def together(batches):
        return jnp.concatenate([b[0] for b in batches], axis=0), [s for b in batches for s in b[1]]

    mine = (record, [lambda w: w])
    shift = [
        moved(mine, lambda w, n=n: ((w[0] - n) % outer, w[1], w[2], w[3])) for n in range(1, outer)
    ]
    other = moved(mine, partner)
    one, two = moved(mine, flip_one), moved(mine, flip_two)

    def names(sources, sender=lambda w: w):
        return [lambda w, s=s: s(sender(w)) for s in sources]

    def chain(*senders):
        def source(w):
            for sender in senders:
                w = sender(w)
            return w

        return source

    shifts = [s for batch in shift for s in batch[1]]
    listed = (
        [lambda w: w, partner, flip_one, flip_two, chain(partner, flip_one), chain(partner, flip_two)]
        + [chain(flip_two, flip_one)] + shifts
        + [chain(partner, flip_two, flip_one)] + names(shifts, partner)
        + names(shifts, flip_one) + names(shifts, flip_two)
        + names(shifts, chain(partner, flip_one)) + names(shifts, chain(partner, flip_two))
        + names(shifts, chain(flip_two, flip_one)) + names(shifts, chain(partner, flip_two, flip_one))
    )
    parts = [[(index(s(w)) // 2, index(s(w)) % 2) for s in listed] for w in everyone]
    assert all(len(set(row)) == len(everyone) for row in parts)
    place = jnp.asarray(np.asarray(parts, np.int32).reshape(-1))
    origin = 0

    def add(state, batches):
        nonlocal origin
        first = origin
        for _, sources in batches:
            for source in sources:
                assert all(source(w) == listed[origin](w) for w in everyone)
                origin += 1
        return spread(state, [batch[0] for batch in batches], place, len(listed), first)

    state = add(None, [mine, other])
    state, (one, two) = after(state, [one, two])
    both = moved(one, flip_two)
    one_partner, two_partner = moved(one, partner), moved(two, partner)
    state = add(state, [one, two])
    state = add(state, [one_partner, two_partner])
    state, (both, *shift) = after(state, [both] + shift)
    shift = together(shift)
    shift_one, shift_two = moved(shift, flip_one), moved(shift, flip_two)
    both_partner, shift_partner = moved(both, partner), moved(shift, partner)
    state = add(state, [both, shift])
    state = add(state, [both_partner, shift_partner])
    state, (shift_one, shift_two) = after(state, [shift_one, shift_two])
    shift_both = moved(shift_one, flip_two)
    one_partner, two_partner = moved(shift_one, partner), moved(shift_two, partner)
    state = add(state, [shift_one, shift_two])
    state, (shift_both,) = after(state, [shift_both])
    both_partner = moved(shift_both, partner)
    state = add(state, [one_partner, two_partner])
    return add(state, [shift_both, both_partner])


def shards(spread_weights, spread_base, qm_base, qm_frac, qm_charge):
    points = GRID
    count_z = lax.axis_size("gz")
    count_y = lax.axis_size("gy")
    devices = count_z * count_y
    z_local = points // count_z
    y_local = points // count_y
    kx_here = -(-(points // 2) // devices)
    here = lax.axis_index("gz") * count_y + lax.axis_index("gy")
    z_rows = round_up(z_local + ORDER - 1 + (0 if z_local % 8 == 0 else 7), 8)
    z_pad = (points - z_local) // 8 * 8 + z_rows
    y_rows = min(round_up(y_local + ORDER - 1, 128), points)

    atoms = spread_weights.shape[1]
    qms = qm_charge.shape[0]
    lines = -(-6 * qms // atoms)
    held = round_up(ORDER**3 + 3 + lines, 8)
    in_stages = count_y == 2 and count_z % 4 == 0
    record = pl.pallas_call(
        record_kernel,
        out_shape=(
            pltpu.VMEM((held, atoms), jnp.float32)
            if in_stages
            else jax.ShapeDtypeStruct((held, atoms), jnp.float32)
        ),
        name="record",
    )(spread_weights, spread_base, qm_base, qm_frac)

    kx_columns, kx_scalars = kx_tables(devices, kx_here, points)
    here_row = here.astype(jnp.int32).reshape(1)
    kx_table = jnp.asarray(kx_columns)
    planes = (count_y, 2 * kx_here, z_pad, y_rows)
    z_need = z_local + ORDER - 1 + (0 if z_local % 8 == 0 else 7)
    smem = pl.BlockSpec(memory_space=pltpu.SMEM)
    hbm = pl.BlockSpec(memory_space=pltpu.HBM)
    vmem = pl.BlockSpec(memory_space=pltpu.VMEM)

    def spread(state, batches, place, listed, origin):
        pieces = [(n, i) for n, array in enumerate(batches) for i in range(array.shape[0] // held)]
        opening = state is None
        return pl.pallas_call(
            lambda *refs: spread_kernel(
                *refs, pieces=pieces, origin=origin, listed=listed, points=points, z_local=z_local,
                y_local=y_local, count_y=count_y, kx_here=kx_here, z_need=z_need, y_rows=y_rows,
                chunk=math.gcd(atoms, 256), opening=opening,
            ),
            grid=(len(pieces),),
            in_specs=[smem, smem, vmem]
            + [hbm] * len(batches)
            + ([] if opening else [vmem, vmem]),
            out_specs=[vmem, vmem],
            out_shape=[pltpu.VMEM(planes, jnp.float32), pltpu.VMEM((devices, 8, qms), jnp.float32)],
            scratch_shapes=[
                pltpu.VMEM((ORDER, 2 * kx_here, atoms), jnp.float32),
                pltpu.VMEM((2, held, atoms), jnp.float32),
                pltpu.SemaphoreType.DMA((2,)),
            ],
            input_output_aliases={} if opening else {3 + len(batches): 0, 4 + len(batches): 1},
            compiler_params=pltpu.CompilerParams(
                dimension_semantics=("arbitrary",), vmem_limit_bytes=VMEM_BYTES
            ),
            cost_estimate=pl.CostEstimate(
                flops=len(pieces) * atoms * ORDER * parts_flops, bytes_accessed=0, transcendentals=0
            ),
            name="spread",
        )(here_row, place, kx_table, *batches, *([] if opening else state))

    parts_flops = 4 * z_rows * 2 * kx_here * y_rows
    if in_stages:
        spread_planes, qm_all = staged(record, count_z // 4, spread)
    else:
        records = lax.all_gather(record, AXES, axis=0, tiled=True)
        order = np.arange(devices)
        place = np.stack([order // count_y, order % count_y], axis=1).astype(np.int32)
        spread_planes, qm_all = spread(None, [records], jnp.asarray(place.reshape(-1)), 0, 0)
    constants = tables(points)
    third = points // RADIX

    def fixed(array):
        return pl.BlockSpec(array.shape, lambda k, n=array.ndim: (0,) * n)

    potential = pl.pallas_call(
        lambda *refs: transform_kernel(
            *refs, points=points, y_local=y_local, count_y=count_y, kx_here=kx_here, third=third
        ),
        grid=(kx_here,),
        in_specs=[smem, smem] + [fixed(array) for array in constants] + [vmem],
        out_specs=vmem,
        out_shape=pltpu.VMEM(planes, jnp.float32),
        input_output_aliases={2 + len(constants): 0},
        compiler_params=pltpu.CompilerParams(
            dimension_semantics=("arbitrary",), vmem_limit_bytes=VMEM_BYTES
        ),
        cost_estimate=pl.CostEstimate(flops=20_000_000_000, bytes_accessed=0, transcendentals=0),
        name="transform",
    )(here_row, jnp.asarray(kx_scalars.reshape(-1)), *constants, spread_planes)

    partial = pl.pallas_call(
        lambda *refs: force_kernel(
            *refs, points=points, z_local=z_local, y_local=y_local, count_y=count_y,
            kx_here=kx_here, z_rows=z_rows,
        ),
        grid=(count_z,),
        in_specs=[smem, vmem, vmem, vmem],
        out_specs=pl.BlockSpec((count_y, 3, qms), lambda p: (p, 0, 0)),
        out_shape=jax.ShapeDtypeStruct((devices, 3, qms), jnp.float32),
        compiler_params=pltpu.CompilerParams(
            dimension_semantics=("arbitrary",), vmem_limit_bytes=VMEM_BYTES
        ),
        name="forces",
    )(here_row, kx_table, qm_all, potential)
    moved = lax.all_to_all(partial, AXES, split_axis=0, concat_axis=0, tiled=True)
    return -qm_charge[None, :] * jnp.sum(moved, axis=0)


def solution(mesh):
    in_specs = (
        P(None, AXES),
        P(None, AXES),
        P(None, AXES),
        P(None, AXES),
        P(AXES),
    )
    out_specs = P(None, AXES)
    return jax.shard_map(shards, mesh=mesh, in_specs=in_specs, out_specs=out_specs, check_vma=False)
```
